32 devices in a mesh: pole: 4 (over x, core), rows: 8 (over z, y).
Axes of the slice: x: 2, y: 2, z: 4, core: 2. Of those that a mesh axis runs over, the one named last changes fastest.
Arguments:
- subspace: float32 [2, 256, 4096], P(None, None, 'rows'), may hold values from -6 to 6
- pivots: float32 [4, 16, 2, 256, 256], P('pole', 'rows'), may hold values from -0.25 to 0.25
- lower_blocks: float32 [4, 16, 2, 256, 256], P('pole', 'rows'), may hold values from -1 to 1
- upper_blocks: float32 [4, 16, 2, 256, 256], P('pole', 'rows'), may hold values from -1 to 1
- pole_weights: float32 [4, 2], P('pole'), may hold values from -4 to 4
Outputs:
- rotated_basis: float32 [2, 256, 4096], P(None, 'pole', 'rows')
The draws below stay inside these ranges and needn't reach their ends.
All inputs are finite; a program needn't handle non-finite values.
Results may differ from the reference program's by a relative error of at most 0.00018.
Values sent between devices are 32-bit elements; how exact they have to be, the bound alone decides.
No kernel may reach another device: no remote copies, remote signals or barrier semaphores. Data moves between devices by JAX's collectives and lax.ppermute only.
A program may use at most 128 MiB of HBM per device.

```python
import jax
import jax.numpy as jnp
from jax import lax

B = 256
M = 256
NS_ITERS = 2
CONTOUR_POLES = 4
BLOCK_ROWS = 16
N = 4096


def decaying(key):
    shape = (CONTOUR_POLES, BLOCK_ROWS, 2, B, B)
    decay_rate = 0.3 ** (1.0 / BLOCK_ROWS)
    spike_key, value_seed_key = jax.random.split(key)
    spike_events = jax.random.bernoulli(spike_key, 0.05, (CONTOUR_POLES, BLOCK_ROWS, 1, 1, 1))
    scale_factor = decay_rate * jnp.where(spike_events, 0.6, 1.0)
    values = jax.random.normal(value_seed_key, shape, jnp.float32)
    values = jnp.clip(values, -6.0, 6.0)
    return (values * scale_factor * (2.0 * B) ** (-0.5)).astype(jnp.float32)


def draw_lower_blocks(key, part):
    return decaying(jax.random.fold_in(key, 11))


def draw_upper_blocks(key, part):
    return decaying(jax.random.fold_in(key, 23))


def block_levels(key, extent, cuts, low, largest):
    gain, own = 1.0, jax.random.fold_in(key, 6)
    for position, parts in cuts:
        steps = jnp.exp(jax.random.uniform(jax.random.fold_in(own, position), (parts,), jnp.float32, low / len(cuts), largest / len(cuts)))
        gain = gain * jnp.repeat(steps, extent[position] // parts).reshape([-1 if axis == position else 1 for axis in range(len(extent))])
    return gain


def centred(key, extent, spread, limit, cuts=(), kind=jnp.bfloat16):
    array = spread * jax.random.normal(key, extent, jnp.float32)
    if cuts:
        array = array * block_levels(key, extent, cuts, -0.22, 0.18)
    return jnp.clip(array, -limit, limit).astype(kind)


def setup_inputs(seed: int = 0) -> dict:
    key_of = jax.random.split(jax.random.key(seed), 6)
    subspace = centred(key_of[0], (2, M, N), 1, 6.0, ((2, 8),), jnp.float32)
    pivots = centred(key_of[1], (CONTOUR_POLES, BLOCK_ROWS, 2, B, B), (2 * B) ** -0.5, 0.25, ((0, 4), (1, 8)), jnp.float32)
    lower_blocks = draw_lower_blocks(jax.random.fold_in(key_of[5], 71), 0)
    upper_blocks = draw_upper_blocks(jax.random.fold_in(key_of[5], 71), 0)
    pole_weights = centred(key_of[4], (CONTOUR_POLES, 2), 1, 4.0, ((0, 4),), jnp.float32)
    return dict(subspace=subspace, pivots=pivots, lower_blocks=lower_blocks, upper_blocks=upper_blocks, pole_weights=pole_weights)


HIGH = lax.Precision.HIGHEST

def real_dot(first, second, dims):
    return lax.dot_general(first, second, (dims, ((), ())), precision=HIGH, preferred_element_type=jnp.float32)

def times_trans(left, matrix):
    dims = ((1,), (1,))
    real = real_dot(left[0], matrix[0], dims) - real_dot(left[1], matrix[1], dims)
    imag = real_dot(left[0], matrix[1], dims) + real_dot(left[1], matrix[0], dims)
    return jnp.stack([real, imag])

def complex_dot(left, right):
    dims = ((1,), (0,))
    real = real_dot(left[0], right[0], dims) - real_dot(left[1], right[1], dims)
    imag = real_dot(left[0], right[1], dims) + real_dot(left[1], right[0], dims)
    return jnp.stack([real, imag])

def gram_matrix(basis):
    dims = ((1,), (1,))
    real = real_dot(basis[0], basis[0], dims) + real_dot(basis[1], basis[1], dims)
    imag = real_dot(basis[0], basis[1], dims) - real_dot(basis[1], basis[0], dims)
    return jnp.stack([real, imag])

def rotate(mixing, basis):
    dims = ((0,), (0,))
    real = real_dot(mixing[0], basis[0], dims) - real_dot(mixing[1], basis[1], dims)
    imag = real_dot(mixing[0], basis[1], dims) + real_dot(mixing[1], basis[0], dims)
    return jnp.stack([real, imag])

def newton_schulz(gram):
    size = gram.shape[1]
    unit = jnp.stack([jnp.eye(size, dtype=jnp.float32), jnp.zeros((size, size), jnp.float32)])
    frob = jnp.sqrt(jnp.sum(gram * gram))
    current = gram / frob
    inverse_root = unit
    for sweep in range(NS_ITERS):
        scale_factor = 1.5 * unit - 0.5 * complex_dot(inverse_root, current)
        current = complex_dot(current, scale_factor)
        inverse_root = complex_dot(scale_factor, inverse_root)
    return (inverse_root, frob)

def reference(subspace, pivots, lower_blocks, upper_blocks, pole_weights):
    pieces = jnp.transpose(subspace.reshape(2, M, BLOCK_ROWS, B), (2, 0, 1, 3))
    blank = jnp.zeros((2, M, B), jnp.float32)
    total = jnp.zeros((2, M, N), jnp.float32)
    for pole in range(CONTOUR_POLES):

        def forward(carry, inputs):
            pivot, lower, piece = inputs
            value = times_trans(piece, pivot) - times_trans(carry, lower)
            return (value, value)

        def backward(carry, inputs):
            value, upper = inputs
            result = value - times_trans(carry, upper)
            return (result, result)
        _, swept = lax.scan(forward, blank, (pivots[pole], lower_blocks[pole], pieces))
        _, solved = lax.scan(backward, blank, (swept, upper_blocks[pole]), reverse=True)
        solution = jnp.transpose(solved, (1, 2, 0, 3)).reshape(2, M, N)
        wreal = pole_weights[pole, 0]
        wimag = pole_weights[pole, 1]
        total = total + jnp.stack([wreal * solution[0] - wimag * solution[1], wreal * solution[1] + wimag * solution[0]])
    gram = gram_matrix(total)
    inverse_root, frob = newton_schulz(gram)
    return rotate(inverse_root, total) * jnp.sqrt(N / frob)
```

```python
import functools

import jax
import jax.numpy as jnp
from jax import lax
from jax.experimental import pallas as pl
from jax.experimental.pallas import tpu as pltpu
from jax.sharding import PartitionSpec as P

NS_ITERS = 2
LANES = 128
HIGH = lax.Precision.HIGH
F32 = jnp.float32


def dot(a, b, dims):
    return lax.dot_general(a, b, (dims, ((), ())), precision=HIGH, preferred_element_type=F32)


def times(left, right, dims):
    real = dot(left[0], right[0], dims) - dot(left[1], right[1], dims)
    imag = dot(left[0], right[1], dims) + dot(left[1], right[0], dims)
    return real, imag


def plain(left, right):
    return times(left, right, ((1,), (0,)))


def trans(left, right):
    return times(left, right, ((1,), (1,)))


def plus(a, b):
    return a[0] + b[0], a[1] + b[1]


def minus(a, b):
    return a[0] - b[0], a[1] - b[1]


def negative(a):
    return -a[0], -a[1]


def pick(choice, a, b):
    return jnp.where(choice, a[0], b[0]), jnp.where(choice, a[1], b[1])


def pair(ref, *index):
    return ref[(*index, 0)], ref[(*index, 1)]


def put(ref, value):
    ref[0] = value[0]
    ref[1] = value[1]


def rows_of(ref, start, size):
    start = pl.multiple_of(start, size)
    return ref[0, pl.ds(start, size), :], ref[1, pl.ds(start, size), :]


def call(body, outs, *args, products=1):
    shapes = [jax.ShapeDtypeStruct(shape, F32) for shape in outs]
    return pl.pallas_call(
        body,
        out_shape=shapes,
        in_specs=[pl.BlockSpec(memory_space=pltpu.VMEM)] * len(args),
        out_specs=[pl.BlockSpec(memory_space=pltpu.VMEM)] * len(outs),
        cost_estimate=pl.CostEstimate(
            flops=products * 3 * 8 * 256**3, bytes_accessed=1 << 20, transcendentals=0
        ),
    )(*args)


def side():
    return lax.rem(lax.axis_index("rows"), 2) == 0


def map_kernel(lower, out):
    count = lower.shape[0]
    value = pair(lower, 0)
    for number in range(1, count):
        value = plain(pair(lower, number), value)
    if count % 2:
        value = negative(value)
    put(out, value)


def back_map_kernel(lower, upper, ahead, out_c, out_r):
    count = upper.shape[0]
    value = pair(upper, count - 1)
    for number in range(count - 2, -1, -1):
        value = plain(pair(upper, number), value)
    if count % 2:
        value = negative(value)
    put(out_c, value)
    levels = [negative(pair(lower, 0))]
    for number in range(1, count - 1):
        levels.append(negative(plain(pair(lower, number), levels[-1])))
    if count > 1:
        levels.append(pair(ahead))
    value = levels[-1]
    for number in range(count - 2, -1, -1):
        value = minus(levels[number], plain(pair(upper, number), value))
    put(out_r, value)


def local_kernel(piece, pivot, lower, upper, states, bkeep, bsend, gkeep, gsend, work):
    count, width = pivot.shape[0], pivot.shape[-1]
    half = bkeep.shape[1]
    mine = jnp.where(side(), 0, half)
    other = half - mine
    last = None
    for number in range(count):
        columns = slice(number * width, (number + 1) * width)
        value = trans((piece[0, :, columns], piece[1, :, columns]), pair(pivot, number))
        if last is not None:
            value = minus(value, trans(last, pair(lower, number)))
        states[number, 0] = value[0]
        states[number, 1] = value[1]
        last = value
    put(bkeep, rows_of(states.at[count - 1], mine, half))
    put(bsend, rows_of(states.at[count - 1], other, half))
    for number in range(count - 2, -1, -1):
        last = minus(pair(states, number), trans(last, pair(upper, number)))
    put(work, last)
    put(gkeep, rows_of(work, mine, half))
    put(gsend, rows_of(work, other, half))


def join_kernel(mine, theirs, bmine, btheirs, out_b, out_a):
    first = side()
    a_first = pick(first, pair(mine), pair(theirs))
    a_second = pick(first, pair(theirs), pair(mine))
    b_first = pick(first, pair(bmine), pair(btheirs))
    b_second = pick(first, pair(btheirs), pair(bmine))
    put(out_b, plus(trans(b_first, a_second), b_second))
    put(out_a, plain(a_second, a_first))


def join_back_kernel(mine, theirs, out):
    first = side()
    c_first = pick(first, pair(mine), pair(theirs))
    c_second = pick(first, pair(theirs), pair(mine))
    put(out, plain(c_first, c_second))


def apply_kernel(state, matrix, base, out):
    put(out, plus(trans(pair(state), pair(matrix)), pair(base)))


def apply_two_kernel(state, matrix, base, more, out):
    value = plus(trans(pair(state), pair(matrix)), pair(base))
    put(out, plus(value, pair(more)))


def turn_kernel(inflow, a_mine, a_theirs, b_mine, b_theirs, r_mine, r_theirs, g_mine, g_theirs,
                c_mine, c_theirs, in_own, in_other, mid, out):
    first = side()
    entering = pair(inflow)
    a_first = pick(first, pair(a_mine), pair(a_theirs))
    b_first = pick(first, pair(b_mine), pair(b_theirs))
    second = plus(trans(entering, a_first), b_first)
    put(in_own, pick(first, entering, second))
    put(in_other, pick(first, second, entering))
    r_second = pick(first, pair(r_theirs), pair(r_mine))
    g_second = pick(first, pair(g_theirs), pair(g_mine))
    middle = plus(g_second, trans(second, r_second))
    put(mid, middle)
    r_first = pick(first, pair(r_mine), pair(r_theirs))
    g_first = pick(first, pair(g_mine), pair(g_theirs))
    c_first = pick(first, pair(c_mine), pair(c_theirs))
    value = plus(g_first, trans(entering, r_first))
    put(out, plus(value, trans(middle, c_first)))


def back_in_kernel(back_inflow, mid, c_mine, c_theirs, own, other):
    first = side()
    c_second = pick(first, pair(c_theirs), pair(c_mine))
    entering = pair(back_inflow)
    first_in = plus(pair(mid), trans(entering, c_second))
    put(own, pick(first, first_in, entering))
    put(other, pick(first, entering, first_in))


def swept_kernel(states, in_own, in_theirs, lower, out, full):
    count = states.shape[0]
    half = in_own.shape[1]
    mine = pl.multiple_of(jnp.where(side(), 0, half), half)
    other = pl.multiple_of(half - mine, half)
    for part in range(2):
        full[part, pl.ds(mine, half), :] = in_own[part]
        full[part, pl.ds(other, half), :] = in_theirs[part]
    carry = pair(full)
    for number in range(count):
        carry = negative(trans(carry, pair(lower, number)))
        out[number, 0] = states[number, 0] + carry[0]
        out[number, 1] = states[number, 1] + carry[1]


def solved_kernel(swept, x_own, x_theirs, upper, weights, keep, send, full):
    count, width = swept.shape[0], swept.shape[-1]
    half = x_own.shape[1]
    mine = pl.multiple_of(jnp.where(side(), 0, half), half)
    other = pl.multiple_of(half - mine, half)
    for part in range(2):
        full[part, pl.ds(mine, half), :] = x_own[part]
        full[part, pl.ds(other, half), :] = x_theirs[part]
    wreal, wimag = weights[0, 0], weights[0, 1]
    carry = pair(full)
    upward = lax.rem(lax.axis_index("pole"), 2) == 1
    for number in range(count - 1, -1, -1):
        carry = minus(pair(swept, number), trans(carry, pair(upper, number)))
        value = (wreal * carry[0] - wimag * carry[1], wreal * carry[1] + wimag * carry[0])
        kept = upward if number >= count // 2 else jnp.logical_not(upward)
        columns = slice((number % (count // 2)) * width, (number % (count // 2) + 1) * width)

        @pl.when(kept)
        def _():
            for part in range(2):
                keep[part, :, columns] = value[part]

        @pl.when(jnp.logical_not(kept))
        def _():
            for part in range(2):
                send[part, :, columns] = value[part]


def halve_kernel(bit, mine, theirs, keep, send):
    width = keep.shape[2]
    up = lax.rem(lax.div(lax.axis_index("pole"), 2**bit), 2) == 1
    for part in range(2):
        low = mine[part, :, :width] + theirs[part, :, :width]
        high = mine[part, :, width:] + theirs[part, :, width:]
        keep[part] = jnp.where(up, high, low)
        send[part] = jnp.where(up, low, high)


def gram_kernel(mine, theirs, total, keep, send, work):
    size = total.shape[1]
    basis = (mine[0] + theirs[0], mine[1] + theirs[1])
    put(total, basis)
    dims = ((1,), (1,))
    real = dot(basis[0], basis[0], dims) + dot(basis[1], basis[1], dims)
    imag = dot(basis[0], basis[1], dims) - dot(basis[1], basis[0], dims)
    row = lax.broadcasted_iota(jnp.int32, (size, size), 0)
    column = lax.broadcasted_iota(jnp.int32, (size, size), 1)
    work[...] = jnp.where(row <= column, real, imag)
    half = size // 2
    start = pl.multiple_of(lax.rem(lax.axis_index("pole"), 2) * half, half)
    keep[...] = work[pl.ds(start, half), :]
    send[...] = work[pl.ds(pl.multiple_of(half - start, half), half), :]


def finish_kernel(states, bits, mine, theirs, *refs):
    pieces, out, held, slab = refs[:-3], refs[-3], refs[-2], refs[-1]
    size = held.shape[0]
    half = size // 2
    pole = lax.axis_index("pole")
    start = pl.multiple_of(lax.rem(pole, 2) * half, half)
    held[pl.ds(start, half), :] = mine[...]
    held[pl.ds(pl.multiple_of(half - start, half), half), :] = theirs[...]
    packed = held[...]
    turned = packed.T
    row = lax.broadcasted_iota(jnp.int32, (size, size), 0)
    column = lax.broadcasted_iota(jnp.int32, (size, size), 1)
    real = jnp.where(row <= column, packed, turned)
    imag = jnp.where(row < column, turned, jnp.where(row > column, -packed, 0.0))
    frob = jnp.sqrt(jnp.sum(real * real + imag * imag, keepdims=True))
    current = (real / frob, imag / frob)
    eye = jnp.where(row == column, 1.0, 0.0)
    columns = out.shape[1]
    inverse = None
    for sweep in range(NS_ITERS):
        both = current if inverse is None else plain(inverse, current)
        factor = (1.5 * eye - 0.5 * both[0], -0.5 * both[1])
        if sweep < NS_ITERS - 1:
            current = plain(current, factor)
            inverse = factor if inverse is None else plain(factor, inverse)
        else:
            put(slab, factor)
            place = pl.multiple_of(pole * columns, columns)
            mixing = (slab[0, pl.ds(place, columns), :], slab[1, pl.ds(place, columns), :])
            if inverse is not None:
                mixing = plain(mixing, inverse)
    factor = jnp.sqrt(states / frob)
    mixing = (mixing[0] * factor, mixing[1] * factor)
    width = pieces[0].shape[2]
    for mask, piece in enumerate(pieces):
        offset = 0
        for bit in range(bits):
            on = lax.rem(lax.div(pole, 2**bit), 2)
            if mask >> bit & 1:
                on = 1 - on
            offset = offset + on * (width << (bits - 1 - bit))
        offset = pl.multiple_of(offset, width)
        value = plain(mixing, pair(piece))
        for part in range(2):
            out[part, :, pl.ds(offset, width)] = value[part]


def shards(subspace, pivots, lower_blocks, upper_blocks, pole_weights):
    devices = lax.axis_size("rows")
    poles = lax.axis_size("pole")
    count, width = pivots.shape[1], pivots.shape[-1]
    vectors = subspace.shape[1]
    half = vectors // 2
    nodes = devices // 2
    pivot, lower, upper = pivots[0], lower_blocks[0], upper_blocks[0]
    square = (2, width, width)
    state = (2, vectors, width)
    strip = (2, half, width)
    vmem = pltpu.VMEM

    def scratch(body, outs, extra, *args, products=1):
        return pl.pallas_call(
            body,
            out_shape=[jax.ShapeDtypeStruct(shape, F32) for shape in outs],
            in_specs=[pl.BlockSpec(memory_space=vmem)] * len(args),
            out_specs=[pl.BlockSpec(memory_space=vmem)] * len(outs),
            scratch_shapes=[vmem(shape, F32) for shape in extra],
            cost_estimate=pl.CostEstimate(
                flops=products * 3 * 8 * 256**3, bytes_accessed=1 << 20, transcendentals=0
            ),
        )(*args)

    swap = [(place, place ^ 1) for place in range(devices)]

    def beside(value):
        return lax.ppermute(value, "rows", swap)

    def between(value, moves):
        return lax.ppermute(
            value, "rows", [(2 * a + s, 2 * b + s) for a, b in moves for s in range(2)]
        )

    def prefix(base, matrix, order):
        if nodes == 4:
            near = between(base, [(order[0], order[1]), (order[2], order[3])])
            ahead = between(matrix, [(order[2], order[3])])
            (passed,) = call(apply_kernel, [strip], near, matrix, base)
            third = between(passed, [(order[1], order[2])])
            fourth = between(passed, [(order[1], order[3])])
            (inflow,) = call(apply_two_kernel, [strip], fourth, ahead, near, third)
            return inflow
        inflow = jnp.zeros(strip, F32)
        for hop in range(nodes - 1):
            (passed,) = call(apply_kernel, [strip], inflow, matrix, base)
            inflow = inflow + between(passed, [(order[hop], order[hop + 1])])
        return inflow

    (a_mine,) = call(map_kernel, [square], lower)
    a_theirs = beside(a_mine)
    states, b_mine, b_send, g_mine, g_send = scratch(
        local_kernel, [(count,) + state, strip, strip, strip, strip], [state],
        subspace, pivot, lower, upper, products=2 * count,
    )
    b_theirs = beside(b_send)
    c_mine, r_mine = call(back_map_kernel, [square, square], lower, upper, a_mine, products=2)
    r_theirs = beside(r_mine)
    g_theirs = beside(g_send)
    c_theirs = beside(c_mine)

    b_node, a_node = call(join_kernel, [strip, square], a_mine, a_theirs, b_mine, b_theirs)
    order = list(range(nodes))
    inflow = prefix(b_node, a_node, order)
    in_own, in_other, mid, g_node = call(
        turn_kernel, [strip] * 4, inflow, a_mine, a_theirs, b_mine, b_theirs,
        r_mine, r_theirs, g_mine, g_theirs, c_mine, c_theirs, products=2,
    )
    (c_node,) = call(join_back_kernel, [square], c_mine, c_theirs)
    back_inflow = prefix(g_node, c_node, order[::-1])
    in_theirs = beside(in_other)
    (swept,) = scratch(
        swept_kernel, [(count,) + state], [state], states, in_own, in_theirs, lower,
        products=count,
    )
    x_own, x_other = call(
        back_in_kernel, [strip] * 2, back_inflow, mid, c_mine, c_theirs
    )
    x_theirs = beside(x_other)

    def over_poles(value, bit):
        return lax.ppermute(value, "pole", [(place, place ^ (1 << bit)) for place in range(poles)])

    columns = count * width
    levels = poles.bit_length() - 1
    bits = levels
    while columns >> bits < LANES:
        bits -= 1
    piece = columns >> 1
    keep, send = pl.pallas_call(
        solved_kernel,
        out_shape=[jax.ShapeDtypeStruct((2, vectors, piece), F32)] * 2,
        in_specs=[pl.BlockSpec(memory_space=vmem)] * 4
        + [pl.BlockSpec(memory_space=pltpu.SMEM)],
        out_specs=[pl.BlockSpec(memory_space=vmem)] * 2,
        scratch_shapes=[vmem(state, F32)],
    )(swept, x_own, x_theirs, upper, pole_weights)
    theirs = over_poles(send, 0)
    for bit in range(1, bits):
        piece >>= 1
        keep, send = call(
            functools.partial(halve_kernel, bit), [(2, vectors, piece)] * 2, keep, theirs
        )
        theirs = over_poles(send, bit)
    for bit in range(bits, levels):
        keep = keep + theirs
        theirs = over_poles(keep, bit)
    total, packed, packed_send = scratch(
        gram_kernel, [(2, vectors, piece), (half, vectors), (half, vectors)],
        [(vectors, vectors)], keep, theirs,
    )
    packed = packed + over_poles(packed_send, 0)
    for bit in range(1, bits):
        packed = packed + over_poles(packed, bit)
    for bit in range(devices.bit_length() - 1):
        packed = packed + lax.ppermute(
            packed, "rows", [(place, place ^ (1 << bit)) for place in range(devices)]
        )
    packed_theirs = over_poles(packed, 0)
    pieces = [total]
    for bit in range(bits):
        pieces = pieces + [over_poles(value, bit) for value in pieces]
    ordered = [None] * len(pieces)
    for index, value in enumerate(pieces):
        ordered[index] = value
    states_in_all = float(columns * devices)
    (result,) = scratch(
        functools.partial(finish_kernel, states_in_all, bits),
        [(2, vectors // poles, columns)], [(vectors, vectors), state],
        packed, packed_theirs, *ordered, products=4,
    )
    return result


def solution(mesh):
    placed = (
        P(None, None, "rows"),
        P("pole", "rows", None, None, None),
        P("pole", "rows", None, None, None),
        P("pole", "rows", None, None, None),
        P("pole", None),
    )
    return jax.shard_map(
        shards, mesh=mesh, in_specs=placed, out_specs=P(None, "pole", "rows"), check_vma=False
    )
```

```python
import functools

import jax
import jax.numpy as jnp
from jax import lax
from jax.experimental import pallas as pl
from jax.experimental.pallas import tpu as pltpu
from jax.sharding import PartitionSpec as P


NS_ITERS = 2
GRANT = 16 << 20
HIGH = lax.Precision.HIGH
F32 = jnp.float32


def dot(a, b, dims):
    return lax.dot_general(a, b, (dims, ((), ())), precision=HIGH, preferred_element_type=F32)


def times(left, right, dims):
    real = dot(left[0], right[0], dims) - dot(left[1], right[1], dims)
    imag = dot(left[0], right[1], dims) + dot(left[1], right[0], dims)
    return real, imag


def plain(left, right):
    return times(left, right, ((1,), (0,)))


def trans(left, right):
    return times(left, right, ((1,), (1,)))


def plus(a, b):
    return a[0] + b[0], a[1] + b[1]


def minus(a, b):
    return a[0] - b[0], a[1] - b[1]


def negative(a):
    return -a[0], -a[1]


def pick(choice, a, b):
    return jnp.where(choice, a[0], b[0]), jnp.where(choice, a[1], b[1])


def pair(ref, *index):
    return ref[(*index, 0)], ref[(*index, 1)]


def put(ref, value):
    ref[0] = value[0]
    ref[1] = value[1]


def rows_of(ref, start, size):
    start = pl.multiple_of(start, size)
    return ref[0, pl.ds(start, size), :], ref[1, pl.ds(start, size), :]


def call(body, outs, *args, products=1):
    shapes = [jax.ShapeDtypeStruct(shape, F32) for shape in outs]
    return pl.pallas_call(
        body,
        out_shape=shapes,
        in_specs=[pl.BlockSpec(memory_space=pltpu.VMEM)] * len(args),
        out_specs=[pl.BlockSpec(memory_space=pltpu.VMEM)] * len(outs),
        cost_estimate=pl.CostEstimate(
            flops=products * 3 * 8 * 256**3, bytes_accessed=1 << 20, transcendentals=0
        ),
        compiler_params=pltpu.CompilerParams(vmem_limit_bytes=GRANT),
    )(*args)


def side():
    return lax.rem(lax.axis_index("rows"), 2) == 0


def map_kernel(lower, out):
    count = lower.shape[0]
    value = pair(lower, 0)
    for number in range(1, count):
        value = plain(pair(lower, number), value)
    if count % 2:
        value = negative(value)
    put(out, value)


def local_kernel(piece, pivot, lower, upper, ahead, states, bkeep, bsend, gkeep, late, work):
    count, width = pivot.shape[0], pivot.shape[-1]
    half = bkeep.shape[1]
    mine = jnp.where(side(), 0, half)
    other = half - mine
    last = None
    for number in range(count):
        columns = slice(number * width, (number + 1) * width)
        value = trans((piece[0, :, columns], piece[1, :, columns]), pair(pivot, number))
        if last is not None:
            value = minus(value, trans(last, pair(lower, number)))
        states[number, 0] = value[0]
        states[number, 1] = value[1]
        last = value
    put(bkeep, rows_of(states.at[count - 1], mine, half))
    put(bsend, rows_of(states.at[count - 1], other, half))
    for number in range(count - 2, -1, -1):
        last = minus(pair(states, number), trans(last, pair(upper, number)))
    put(work, last)
    put(gkeep, rows_of(work, mine, half))
    value = rows_of(work, other, half)
    for part in range(2):
        late[part, 2 * width :, :] = value[part]
    levels = [negative(pair(lower, 0))]
    for number in range(1, count - 1):
        levels.append(negative(plain(pair(lower, number), levels[-1])))
    if count > 1:
        levels.append(pair(ahead))
    value = levels[-1]
    for number in range(count - 2, -1, -1):
        value = minus(levels[number], plain(pair(upper, number), value))
    for part in range(2):
        late[part, :width, :] = value[part]
    value = pair(upper, count - 1)
    for number in range(count - 2, -1, -1):
        value = plain(pair(upper, number), value)
    if count % 2:
        value = negative(value)
    for part in range(2):
        late[part, width : 2 * width, :] = value[part]


def part_of(ref, start, size):
    return ref[0, start : start + size, :], ref[1, start : start + size, :]


def join_kernel(mine, theirs, bmine, btheirs, out_b, out_a):
    first = side()
    a_first = pick(first, pair(mine), pair(theirs))
    a_second = pick(first, pair(theirs), pair(mine))
    b_first = pick(first, pair(bmine), pair(btheirs))
    b_second = pick(first, pair(btheirs), pair(bmine))
    put(out_b, plus(trans(b_first, a_second), b_second))
    put(out_a, plain(a_second, a_first))


def join_back_kernel(mine, theirs, out):
    first = side()
    size = out.shape[1]
    c_first = pick(first, part_of(mine, size, size), part_of(theirs, size, size))
    c_second = pick(first, part_of(theirs, size, size), part_of(mine, size, size))
    put(out, plain(c_first, c_second))


def apply_kernel(state, matrix, base, out):
    put(out, plus(trans(pair(state), pair(matrix)), pair(base)))


def turn_kernel(inflow, a_mine, a_theirs, b_mine, b_theirs, g_mine, late_mine, late_theirs,
                in_own, in_other, mid, out):
    first = side()
    size = a_mine.shape[1]
    half = inflow.shape[1]
    entering = pair(inflow)
    a_first = pick(first, pair(a_mine), pair(a_theirs))
    b_first = pick(first, pair(b_mine), pair(b_theirs))
    second = plus(trans(entering, a_first), b_first)
    put(in_own, pick(first, entering, second))
    put(in_other, pick(first, second, entering))
    r_mine, r_theirs = part_of(late_mine, 0, size), part_of(late_theirs, 0, size)
    c_mine, c_theirs = part_of(late_mine, size, size), part_of(late_theirs, size, size)
    g_own, g_theirs = pair(g_mine), part_of(late_theirs, 2 * size, half)
    middle = plus(pick(first, g_theirs, g_own), trans(second, pick(first, r_theirs, r_mine)))
    put(mid, middle)
    value = plus(pick(first, g_own, g_theirs), trans(entering, pick(first, r_mine, r_theirs)))
    put(out, plus(value, trans(middle, pick(first, c_mine, c_theirs))))


def back_in_kernel(back_inflow, mid, late_mine, late_theirs, own, other):
    first = side()
    size = back_inflow.shape[2]
    c_mine, c_theirs = part_of(late_mine, size, size), part_of(late_theirs, size, size)
    entering = pair(back_inflow)
    first_in = plus(pair(mid), trans(entering, pick(first, c_theirs, c_mine)))
    put(own, pick(first, first_in, entering))
    put(other, pick(first, entering, first_in))


def swept_kernel(states, in_own, in_theirs, lower, out_own, out_theirs):
    count = states.shape[0]
    half = in_own.shape[1]
    mine = jnp.where(side(), 0, half)
    for carry, start, out in ((in_own, mine, out_own), (in_theirs, half - mine, out_theirs)):
        carry = pair(carry)
        for number in range(count):
            carry = negative(trans(carry, pair(lower, number)))
            put(out.at[number], plus(rows_of(states.at[number], start, half), carry))


def solved_kernel(swept, entering, upper, weights, keep, send):
    count, width = swept.shape[0], swept.shape[-1]
    wreal, wimag = weights[0, 0], weights[0, 1]
    carry = pair(entering)
    upward = lax.rem(lax.axis_index("pole"), 2) == 1
    for number in range(count - 1, -1, -1):
        carry = minus(pair(swept, number), trans(carry, pair(upper, number)))
        value = (wreal * carry[0] - wimag * carry[1], wreal * carry[1] + wimag * carry[0])
        kept = upward if number >= count // 2 else jnp.logical_not(upward)
        columns = slice((number % (count // 2)) * width, (number % (count // 2) + 1) * width)

        @pl.when(kept)
        def _():
            for part in range(2):
                keep[part, :, columns] = value[part]

        @pl.when(jnp.logical_not(kept))
        def _():
            for part in range(2):
                send[part, :, columns] = value[part]


def gram_kernel(own, own_more, theirs, theirs_more, total, keep, send, work):
    size = total.shape[1]
    half = size // 2
    mine = jnp.where(side(), 0, half)
    for first, second, start in ((own, own_more, mine), (theirs, theirs_more, half - mine)):
        start = pl.multiple_of(start, half)
        for part in range(2):
            total[part, pl.ds(start, half), :] = first[part] + second[part]
    basis = pair(total)
    dims = ((1,), (1,))
    real = dot(basis[0], basis[0], dims) + dot(basis[1], basis[1], dims)
    imag = dot(basis[0], basis[1], dims) - dot(basis[1], basis[0], dims)
    row = lax.broadcasted_iota(jnp.int32, (size, size), 0)
    column = lax.broadcasted_iota(jnp.int32, (size, size), 1)
    work[...] = jnp.where(row <= column, real, imag)
    start = pl.multiple_of(lax.rem(lax.axis_index("pole"), 2) * half, half)
    keep[...] = work[pl.ds(start, half), :]
    send[...] = work[pl.ds(pl.multiple_of(half - start, half), half), :]


def finish_kernel(states, mine, theirs, q_mine, q_theirs, out, held, slab):
    size = held.shape[0]
    half = size // 2
    pole = lax.axis_index("pole")
    start = pl.multiple_of(lax.rem(pole, 2) * half, half)
    held[pl.ds(start, half), :] = mine[...]
    held[pl.ds(pl.multiple_of(half - start, half), half), :] = theirs[...]
    packed = held[...]
    turned = packed.T
    row = lax.broadcasted_iota(jnp.int32, (size, size), 0)
    column = lax.broadcasted_iota(jnp.int32, (size, size), 1)
    real = jnp.where(row <= column, packed, turned)
    imag = jnp.where(row < column, turned, jnp.where(row > column, -packed, 0.0))
    frob = jnp.sqrt(jnp.sum(real * real + imag * imag, keepdims=True))
    current = (real / frob, imag / frob)
    eye = jnp.where(row == column, 1.0, 0.0)
    columns = out.shape[1]
    inverse = None
    for sweep in range(NS_ITERS):
        both = current if inverse is None else plain(inverse, current)
        factor = (1.5 * eye - 0.5 * both[0], -0.5 * both[1])
        if sweep < NS_ITERS - 1:
            current = plain(current, factor)
            inverse = factor if inverse is None else plain(factor, inverse)
        else:
            put(slab, factor)
            place = pl.multiple_of(pole * columns, columns)
            mixing = (slab[0, pl.ds(place, columns), :], slab[1, pl.ds(place, columns), :])
            if inverse is not None:
                mixing = plain(mixing, inverse)
    factor = jnp.sqrt(states / frob)
    mixing = (mixing[0] * factor, mixing[1] * factor)
    width = q_mine.shape[2]
    place = lax.rem(pole, 2) * width
    for piece, offset in ((q_mine, place), (q_theirs, width - place)):
        value = plain(mixing, pair(piece))
        for part in range(2):
            out[part, :, pl.ds(pl.multiple_of(offset, width), width)] = value[part]


def shards(subspace, pivots, lower_blocks, upper_blocks, pole_weights):
    devices = lax.axis_size("rows")
    poles = lax.axis_size("pole")
    count, width = pivots.shape[1], pivots.shape[-1]
    vectors = subspace.shape[1]
    half = vectors // 2
    nodes = devices // 2
    pivot, lower, upper = pivots[0], lower_blocks[0], upper_blocks[0]
    square = (2, width, width)
    state = (2, vectors, width)
    strip = (2, half, width)
    vmem = pltpu.VMEM

    def scratch(body, outs, extra, *args, products=1):
        return pl.pallas_call(
            body,
            out_shape=[jax.ShapeDtypeStruct(shape, F32) for shape in outs],
            in_specs=[pl.BlockSpec(memory_space=vmem)] * len(args),
            out_specs=[pl.BlockSpec(memory_space=vmem)] * len(outs),
            scratch_shapes=[vmem(shape, F32) for shape in extra],
            cost_estimate=pl.CostEstimate(
                flops=products * 3 * 8 * 256**3, bytes_accessed=1 << 20, transcendentals=0
            ),
            compiler_params=pltpu.CompilerParams(vmem_limit_bytes=GRANT),
        )(*args)

    swap = [(place, place ^ 1) for place in range(devices)]

    def beside(value):
        return lax.ppermute(value, "rows", swap)

    def between(value, moves):
        return lax.ppermute(
            value, "rows", [(2 * a + s, 2 * b + s) for a, b in moves for s in range(2)]
        )

    def prefix(base, matrix, order):
        inflow = None
        for hop in range(nodes - 1):
            passed = base
            if hop:
                (passed,) = call(apply_kernel, [strip], inflow, matrix, base)
            came = between(passed, [(order[hop], order[hop + 1])])
            inflow = came if inflow is None else inflow + came
        return jnp.zeros(strip, F32) if inflow is None else inflow

    (a_mine,) = call(map_kernel, [square], lower)
    a_theirs = beside(a_mine)
    states, b_mine, b_send, g_mine, late_mine = scratch(
        local_kernel, [(count,) + state, strip, strip, strip, (2, 2 * width + half, width)],
        [state], subspace, pivot, lower, upper, a_mine, products=2 * count + 3,
    )
    b_theirs = beside(b_send)
    late_theirs = beside(late_mine)

    b_node, a_node = call(join_kernel, [strip, square], a_mine, a_theirs, b_mine, b_theirs)
    order = list(range(nodes))
    inflow = prefix(b_node, a_node, order)
    in_own, in_other, mid, g_node = call(
        turn_kernel, [strip] * 4, inflow, a_mine, a_theirs, b_mine, b_theirs,
        g_mine, late_mine, late_theirs, products=2,
    )
    (c_node,) = call(join_back_kernel, [square], late_mine, late_theirs)
    back_inflow = prefix(g_node, c_node, order[::-1])
    in_theirs = beside(in_other)
    swept_own, swept_theirs = call(
        swept_kernel, [(count,) + strip] * 2, states, in_own, in_theirs, lower, products=count
    )
    x_own, x_other = call(
        back_in_kernel, [strip] * 2, back_inflow, mid, late_mine, late_theirs
    )
    x_theirs = beside(x_other)

    def over_poles(value, bit):
        return lax.ppermute(value, "pole", [(place, place ^ (1 << bit)) for place in range(poles)])

    levels = poles.bit_length() - 1
    columns = count * width
    block = (2, half, columns // 2)

    def poled(swept, entering):
        keep, send = pl.pallas_call(
            solved_kernel,
            out_shape=[jax.ShapeDtypeStruct(block, F32)] * 2,
            in_specs=[pl.BlockSpec(memory_space=vmem)] * 3
            + [pl.BlockSpec(memory_space=pltpu.SMEM)],
            out_specs=[pl.BlockSpec(memory_space=vmem)] * 2,
            compiler_params=pltpu.CompilerParams(vmem_limit_bytes=GRANT),
        )(swept, entering, upper, pole_weights)
        value, more = keep, over_poles(send, 0)
        for bit in range(1, levels):
            value = value + more
            more = over_poles(value, bit)
        return value, more

    own, own_more = poled(swept_own, x_own)
    theirs, theirs_more = poled(swept_theirs, x_theirs)
    total, packed, packed_send = scratch(
        gram_kernel, [(2, vectors, columns // 2), (half, vectors), (half, vectors)],
        [(vectors, vectors)], own, own_more, theirs, theirs_more,
    )
    packed = packed + over_poles(packed_send, 0)
    for bit in range(devices.bit_length() - 1):
        packed = packed + lax.ppermute(
            packed, "rows", [(place, place ^ (1 << bit)) for place in range(devices)]
        )
    packed_theirs = over_poles(packed, 0)
    total_theirs = over_poles(total, 0)
    (result,) = scratch(
        functools.partial(finish_kernel, float(columns * devices)),
        [(2, vectors // poles, columns)], [(vectors, vectors), state],
        packed, packed_theirs, total, total_theirs, products=4,
    )
    return result


def solution(mesh):
    placed = (
        P(None, None, "rows"),
        P("pole", "rows", None, None, None),
        P("pole", "rows", None, None, None),
        P("pole", "rows", None, None, None),
        P("pole", None),
    )
    return jax.shard_map(
        shards, mesh=mesh, in_specs=placed, out_specs=P(None, "pole", "rows"), check_vma=False
    )
```

```python
import functools

import jax
import jax.numpy as jnp
from jax import lax
from jax.experimental import pallas as pl
from jax.experimental.pallas import tpu as pltpu
from jax.sharding import PartitionSpec as P


NS_ITERS = 2
GRANT = 8 << 20
HIGH = lax.Precision.HIGH
F32 = jnp.float32


def dot(a, b, dims):
    return lax.dot_general(a, b, (dims, ((), ())), precision=HIGH, preferred_element_type=F32)


def times(left, right, dims):
    real = dot(left[0], right[0], dims) - dot(left[1], right[1], dims)
    imag = dot(left[0], right[1], dims) + dot(left[1], right[0], dims)
    return real, imag


def plain(left, right):
    return times(left, right, ((1,), (0,)))


def trans(left, right):
    return times(left, right, ((1,), (1,)))


def plus(a, b):
    return a[0] + b[0], a[1] + b[1]


def minus(a, b):
    return a[0] - b[0], a[1] - b[1]


def negative(a):
    return -a[0], -a[1]


def pick(choice, a, b):
    return jnp.where(choice, a[0], b[0]), jnp.where(choice, a[1], b[1])


def pair(ref, *index):
    return ref[(*index, 0)], ref[(*index, 1)]


def put(ref, value):
    ref[0] = value[0]
    ref[1] = value[1]


def rows_of(ref, start, size):
    start = pl.multiple_of(start, size)
    return ref[0, pl.ds(start, size), :], ref[1, pl.ds(start, size), :]


def call(body, outs, *args, products=1):
    shapes = [jax.ShapeDtypeStruct(shape, F32) for shape in outs]
    return pl.pallas_call(
        body,
        out_shape=shapes,
        in_specs=[pl.BlockSpec(memory_space=pltpu.VMEM)] * len(args),
        out_specs=[pl.BlockSpec(memory_space=pltpu.VMEM)] * len(outs),
        cost_estimate=pl.CostEstimate(
            flops=products * 3 * 8 * 256**3, bytes_accessed=1 << 20, transcendentals=0
        ),
        compiler_params=pltpu.CompilerParams(vmem_limit_bytes=GRANT),
    )(*args)


def side():
    return lax.rem(lax.axis_index("rows"), 2) == 0


def map_kernel(lower, out):
    count = lower.shape[0]
    value = pair(lower, 0)
    for number in range(1, count):
        value = plain(pair(lower, number), value)
    if count % 2:
        value = negative(value)
    put(out, value)


def local_kernel(piece, pivot, lower, upper, ahead, states, bkeep, bsend, gkeep, cmap, late, work):
    count, width = pivot.shape[0], pivot.shape[-1]
    half = bkeep.shape[1]
    mine = jnp.where(side(), 0, half)
    other = half - mine
    last = None
    for number in range(count):
        columns = slice(number * width, (number + 1) * width)
        value = trans((piece[0, :, columns], piece[1, :, columns]), pair(pivot, number))
        if last is not None:
            value = minus(value, trans(last, pair(lower, number)))
        states[number, 0] = value[0]
        states[number, 1] = value[1]
        last = value
    put(bkeep, rows_of(states.at[count - 1], mine, half))
    put(bsend, rows_of(states.at[count - 1], other, half))
    for number in range(count - 2, -1, -1):
        last = minus(pair(states, number), trans(last, pair(upper, number)))
    put(work, last)
    put(gkeep, rows_of(work, mine, half))
    value = rows_of(work, other, half)
    for part in range(2):
        late[part, width:, :] = value[part]
    levels = [negative(pair(lower, 0))]
    for number in range(1, count - 1):
        levels.append(negative(plain(pair(lower, number), levels[-1])))
    if count > 1:
        levels.append(pair(ahead))
    value = levels[-1]
    for number in range(count - 2, -1, -1):
        value = minus(levels[number], plain(pair(upper, number), value))
    for part in range(2):
        late[part, :width, :] = value[part]
    value = pair(upper, count - 1)
    for number in range(count - 2, -1, -1):
        value = plain(pair(upper, number), value)
    if count % 2:
        value = negative(value)
    put(cmap, value)


def part_of(ref, start, size):
    return ref[0, start : start + size, :], ref[1, start : start + size, :]


def join_kernel(mine, theirs, bmine, btheirs, out_b, out_a):
    first = side()
    a_first = pick(first, pair(mine), pair(theirs))
    a_second = pick(first, pair(theirs), pair(mine))
    b_first = pick(first, pair(bmine), pair(btheirs))
    b_second = pick(first, pair(btheirs), pair(bmine))
    put(out_b, plus(trans(b_first, a_second), b_second))
    put(out_a, plain(a_second, a_first))


def join_back_kernel(mine, theirs, out):
    first = side()
    c_first = pick(first, pair(mine), pair(theirs))
    c_second = pick(first, pair(theirs), pair(mine))
    put(out, plain(c_first, c_second))


def apply_kernel(state, matrix, base, out):
    put(out, plus(trans(pair(state), pair(matrix)), pair(base)))


def turn_kernel(inflow, a_mine, a_theirs, b_mine, b_theirs, g_mine, late_mine, late_theirs,
                c_mine, c_theirs, in_own, in_other, mid, *outs):
    first = side()
    size = a_mine.shape[1]
    half = inflow.shape[1]
    entering = pair(inflow)
    a_first = pick(first, pair(a_mine), pair(a_theirs))
    b_first = pick(first, pair(b_mine), pair(b_theirs))
    second = plus(trans(entering, a_first), b_first)
    put(in_own, pick(first, entering, second))
    put(in_other, pick(first, second, entering))
    r_mine, r_theirs = part_of(late_mine, 0, size), part_of(late_theirs, 0, size)
    g_own, g_theirs = pair(g_mine), part_of(late_theirs, size, half)
    middle = plus(pick(first, g_theirs, g_own), trans(second, pick(first, r_theirs, r_mine)))
    put(mid, middle)
    value = plus(pick(first, g_own, g_theirs), trans(entering, pick(first, r_mine, r_theirs)))
    value = plus(value, trans(middle, pick(first, pair(c_mine), pair(c_theirs))))
    if len(outs) == 1:
        put(outs[0], value)
        return
    quarter = half // 2
    low = (value[0][:quarter], value[1][:quarter])
    high = (value[0][quarter:], value[1][quarter:])
    source = back_place(4) == 0
    put(outs[0], pick(source, low, high))
    put(outs[1], pick(source, high, low))


def back_place(nodes):
    return nodes - 1 - lax.div(lax.axis_index("rows"), 2)


def middle_kernel(mine_a, mine_b, came_a, came_b, c_mine, c_other, keep, send, last):
    place = back_place(4)
    one = place == 1
    c_one = pick(one, pair(c_mine), pair(c_other))
    c_two = pick(one, pair(c_other), pair(c_mine))
    start = pick(one, pair(came_a), pair(came_b))
    second = plus(trans(start, c_one), pick(one, pair(mine_b), pair(came_a)))
    third = plus(trans(second, c_two), pick(one, pair(came_b), pair(mine_a)))
    put(keep, pick(one, start, second))
    put(send, pick(place == 0, pair(mine_b), pick(one, second, third)))
    put(last, third)


def back_in(entering, mid, c_mine, c_theirs, own, other):
    first = side()
    first_in = plus(pair(mid), trans(entering, pick(first, pair(c_theirs), pair(c_mine))))
    put(own, pick(first, first_in, entering))
    put(other, pick(first, entering, first_in))


def back_in_kernel(back_inflow, *refs):
    back_in(pair(back_inflow), *refs)


def back_in_parts_kernel(keep, came, last, mid, c_mine, c_theirs, own, other, work):
    place = back_place(4)
    low = pick(place == 1, pair(keep), pick(place == 2, pair(came), pair(last)))
    high = pick(place == 2, pair(keep), pair(came))
    quarter = keep.shape[1]
    for part in range(2):
        work[part, :quarter] = low[part]
        work[part, quarter:] = high[part]
    back_in(pair(work), mid, c_mine, c_theirs, own, other)


def swept_kernel(states, in_own, in_theirs, lower, out_own, out_theirs):
    count = states.shape[0]
    half = in_own.shape[1]
    mine = jnp.where(side(), 0, half)
    for carry, start, out in ((in_own, mine, out_own), (in_theirs, half - mine, out_theirs)):
        carry = pair(carry)
        for number in range(count):
            carry = negative(trans(carry, pair(lower, number)))
            put(out.at[number], plus(rows_of(states.at[number], start, half), carry))


def solved_kernel(swept, entering, upper, weights, keep, send):
    count, width = swept.shape[0], swept.shape[-1]
    wreal, wimag = weights[0, 0], weights[0, 1]
    carry = pair(entering)
    upward = lax.rem(lax.axis_index("pole"), 2) == 1
    for number in range(count - 1, -1, -1):
        carry = minus(pair(swept, number), trans(carry, pair(upper, number)))
        value = (wreal * carry[0] - wimag * carry[1], wreal * carry[1] + wimag * carry[0])
        kept = upward if number >= count // 2 else jnp.logical_not(upward)
        columns = slice((number % (count // 2)) * width, (number % (count // 2) + 1) * width)

        @pl.when(kept)
        def _():
            for part in range(2):
                keep[part, :, columns] = value[part]

        @pl.when(jnp.logical_not(kept))
        def _():
            for part in range(2):
                send[part, :, columns] = value[part]


def gram_kernel(own, own_more, theirs, theirs_more, total, keep, send, work):
    size = total.shape[1]
    half = size // 2
    mine = jnp.where(side(), 0, half)
    for first, second, start in ((own, own_more, mine), (theirs, theirs_more, half - mine)):
        start = pl.multiple_of(start, half)
        for part in range(2):
            total[part, pl.ds(start, half), :] = first[part] + second[part]
    basis = pair(total)
    dims = ((1,), (1,))
    real = dot(basis[0], basis[0], dims) + dot(basis[1], basis[1], dims)
    imag = dot(basis[0], basis[1], dims) - dot(basis[1], basis[0], dims)
    row = lax.broadcasted_iota(jnp.int32, (size, size), 0)
    column = lax.broadcasted_iota(jnp.int32, (size, size), 1)
    work[...] = jnp.where(row <= column, real, imag)
    start = pl.multiple_of(lax.rem(lax.axis_index("pole"), 2) * half, half)
    keep[...] = work[pl.ds(start, half), :]
    send[...] = work[pl.ds(pl.multiple_of(half - start, half), half), :]


def finish_kernel(states, mine, theirs, q_mine, q_theirs, out, held, slab):
    size = held.shape[0]
    half = size // 2
    pole = lax.axis_index("pole")
    start = pl.multiple_of(lax.rem(pole, 2) * half, half)
    held[pl.ds(start, half), :] = mine[...]
    held[pl.ds(pl.multiple_of(half - start, half), half), :] = theirs[...]
    packed = held[...]
    turned = packed.T
    row = lax.broadcasted_iota(jnp.int32, (size, size), 0)
    column = lax.broadcasted_iota(jnp.int32, (size, size), 1)
    real = jnp.where(row <= column, packed, turned)
    imag = jnp.where(row < column, turned, jnp.where(row > column, -packed, 0.0))
    frob = jnp.sqrt(jnp.sum(real * real + imag * imag, keepdims=True))
    current = (real / frob, imag / frob)
    eye = jnp.where(row == column, 1.0, 0.0)
    columns = out.shape[1]
    inverse = None
    for sweep in range(NS_ITERS):
        both = current if inverse is None else plain(inverse, current)
        factor = (1.5 * eye - 0.5 * both[0], -0.5 * both[1])
        if sweep < NS_ITERS - 1:
            current = plain(current, factor)
            inverse = factor if inverse is None else plain(factor, inverse)
        else:
            put(slab, factor)
            place = pl.multiple_of(pole * columns, columns)
            mixing = (slab[0, pl.ds(place, columns), :], slab[1, pl.ds(place, columns), :])
            if inverse is not None:
                mixing = plain(mixing, inverse)
    factor = jnp.sqrt(states / frob)
    mixing = (mixing[0] * factor, mixing[1] * factor)
    width = q_mine.shape[2]
    place = lax.rem(pole, 2) * width
    for piece, offset in ((q_mine, place), (q_theirs, width - place)):
        value = plain(mixing, pair(piece))
        for part in range(2):
            out[part, :, pl.ds(pl.multiple_of(offset, width), width)] = value[part]


def shards(subspace, pivots, lower_blocks, upper_blocks, pole_weights):
    devices = lax.axis_size("rows")
    poles = lax.axis_size("pole")
    count, width = pivots.shape[1], pivots.shape[-1]
    vectors = subspace.shape[1]
    half = vectors // 2
    nodes = devices // 2
    pivot, lower, upper = pivots[0], lower_blocks[0], upper_blocks[0]
    square = (2, width, width)
    state = (2, vectors, width)
    strip = (2, half, width)
    vmem = pltpu.VMEM

    def scratch(body, outs, extra, *args, products=1):
        return pl.pallas_call(
            body,
            out_shape=[jax.ShapeDtypeStruct(shape, F32) for shape in outs],
            in_specs=[pl.BlockSpec(memory_space=vmem)] * len(args),
            out_specs=[pl.BlockSpec(memory_space=vmem)] * len(outs),
            scratch_shapes=[vmem(shape, F32) for shape in extra],
            cost_estimate=pl.CostEstimate(
                flops=products * 3 * 8 * 256**3, bytes_accessed=1 << 20, transcendentals=0
            ),
            compiler_params=pltpu.CompilerParams(vmem_limit_bytes=GRANT),
        )(*args)

    swap = [(place, place ^ 1) for place in range(devices)]

    def beside(value):
        return lax.ppermute(value, "rows", swap)

    def between(value, moves):
        return lax.ppermute(
            value, "rows", [(2 * a + s, 2 * b + s) for a, b in moves for s in range(2)]
        )

    def prefix(base, matrix, order):
        inflow = None
        for hop in range(nodes - 1):
            passed = base
            if hop:
                (passed,) = call(apply_kernel, [strip], inflow, matrix, base)
            came = between(passed, [(order[hop], order[hop + 1])])
            inflow = came if inflow is None else inflow + came
        return jnp.zeros(strip, F32) if inflow is None else inflow

    (a_mine,) = call(map_kernel, [square], lower)
    a_theirs = beside(a_mine)
    states, b_mine, b_send, g_mine, c_mine, late_mine = scratch(
        local_kernel,
        [(count,) + state, strip, strip, strip, square, (2, width + half, width)],
        [state], subspace, pivot, lower, upper, a_mine, products=2 * count + 3,
    )
    b_theirs = beside(b_send)
    c_theirs = beside(c_mine)
    late_theirs = beside(late_mine)

    b_node, a_node = call(join_kernel, [strip, square], a_mine, a_theirs, b_mine, b_theirs)
    order = list(range(nodes))
    inflow = prefix(b_node, a_node, order)
    (c_node,) = call(join_back_kernel, [square], c_mine, c_theirs)
    quarter = (2, half // 2, width)
    short = nodes == 4
    in_own, in_other, mid, *ends = call(
        turn_kernel, [strip] * 3 + ([quarter] * 2 if short else [strip]), inflow, a_mine, a_theirs,
        b_mine, b_theirs, g_mine, late_mine, late_theirs, c_mine, c_theirs, products=2,
    )
    if short:
        c_other = between(c_node, [(1, 2), (2, 1)])
        came_a = between(ends[0], [(3, 2), (2, 1)])
        came_b = between(ends[1], [(3, 1), (1, 2)])
        keep, send, last = call(
            middle_kernel, [quarter] * 3, *ends, came_a, came_b, c_node, c_other
        )
        came = between(send, [(3, 2), (2, 1), (1, 0)])
        last = between(last, [(2, 0)])
    else:
        back_inflow = prefix(ends[0], c_node, order[::-1])
    in_theirs = beside(in_other)
    swept_own, swept_theirs = call(
        swept_kernel, [(count,) + strip] * 2, states, in_own, in_theirs, lower,
        products=count,
    )
    if short:
        x_own, x_other = scratch(
            back_in_parts_kernel, [strip] * 2, [strip], keep, came, last, mid, c_mine, c_theirs
        )
    else:
        x_own, x_other = call(
            back_in_kernel, [strip] * 2, back_inflow, mid, c_mine, c_theirs
        )
    x_theirs = beside(x_other)

    def over_poles(value, bit):
        return lax.ppermute(value, "pole", [(place, place ^ (1 << bit)) for place in range(poles)])

    levels = poles.bit_length() - 1
    columns = count * width
    block = (2, half, columns // 2)

    def poled(swept, entering):
        keep, send = pl.pallas_call(
            solved_kernel,
            out_shape=[jax.ShapeDtypeStruct(block, F32)] * 2,
            in_specs=[pl.BlockSpec(memory_space=vmem)] * 3
            + [pl.BlockSpec(memory_space=pltpu.SMEM)],
            out_specs=[pl.BlockSpec(memory_space=vmem)] * 2,
            compiler_params=pltpu.CompilerParams(vmem_limit_bytes=GRANT),
        )(swept, entering, upper, pole_weights)
        value, more = keep, over_poles(send, 0)
        for bit in range(1, levels):
            value = value + more
            more = over_poles(value, bit)
        return value, more

    own, own_more = poled(swept_own, x_own)
    theirs, theirs_more = poled(swept_theirs, x_theirs)
    total, packed, packed_send = scratch(
        gram_kernel, [(2, vectors, columns // 2), (half, vectors), (half, vectors)],
        [(vectors, vectors)], own, own_more, theirs, theirs_more,
    )
    packed = packed + over_poles(packed_send, 0)
    for bit in range(devices.bit_length() - 1):
        packed = packed + lax.ppermute(
            packed, "rows", [(place, place ^ (1 << bit)) for place in range(devices)]
        )
    packed_theirs = over_poles(packed, 0)
    total_theirs = over_poles(total, 0)
    (result,) = scratch(
        functools.partial(finish_kernel, float(columns * devices)),
        [(2, vectors // poles, columns)], [(vectors, vectors), state],
        packed, packed_theirs, total, total_theirs, products=4,
    )
    return result


def solution(mesh):
    placed = (
        P(None, None, "rows"),
        P("pole", "rows", None, None, None),
        P("pole", "rows", None, None, None),
        P("pole", "rows", None, None, None),
        P("pole", None),
    )
    return jax.shard_map(
        shards, mesh=mesh, in_specs=placed, out_specs=P(None, "pole", "rows"), check_vma=False
    )
```

```python
import functools

import jax
import jax.numpy as jnp
from jax import lax
from jax.experimental import pallas as pl
from jax.experimental.pallas import tpu as pltpu
from jax.sharding import PartitionSpec as P


GRANT = 8 << 20
LANES = 128
HIGH = lax.Precision.HIGH
F32 = jnp.float32


def dot(a, b, dims, precision=None):
    return lax.dot_general(
        a, b, (dims, ((), ())), precision=precision, preferred_element_type=F32
    )


def halves(a):
    high = a.astype(jnp.bfloat16)
    return high, (a - high.astype(F32)).astype(jnp.bfloat16)


def stacked(value):
    real, imag = halves(value[0]), halves(value[1])
    high = jnp.concatenate([real[0], imag[0]], axis=0)
    return high, jnp.concatenate([high, real[1], imag[1]], axis=0)


def against(left, part, dims):
    high, both = left
    size = high.shape[0]
    wide = dot(both, part[0], dims)
    value = wide[:size] + (wide[size:] + dot(high, part[1], dims))
    return value[: size // 2], value[size // 2 :]


def few(left, parts, dims):
    left = stacked(left)
    with_real, with_imag = against(left, parts[0], dims), against(left, parts[1], dims)
    return with_real[0] - with_imag[1], with_imag[0] + with_real[1]


def times(left, right, dims):
    rows = left[0].shape[0]
    if rows <= LANES // 2 or (rows <= LANES and dims[1] == (1,)):
        return few(left, (halves(right[0]), halves(right[1])), dims)
    real = dot(left[0], right[0], dims, HIGH) - dot(left[1], right[1], dims, HIGH)
    imag = dot(left[0], right[1], dims, HIGH) + dot(left[1], right[0], dims, HIGH)
    return real, imag


def plain(left, right):
    return times(left, right, ((1,), (0,)))


def trans(left, right):
    return times(left, right, ((1,), (1,)))


def plus(a, b):
    return a[0] + b[0], a[1] + b[1]


def minus(a, b):
    return a[0] - b[0], a[1] - b[1]


def negative(a):
    return -a[0], -a[1]


def pick(choice, a, b):
    return jnp.where(choice, a[0], b[0]), jnp.where(choice, a[1], b[1])


def pair(ref, *index):
    return ref[(*index, 0)], ref[(*index, 1)]


def put(ref, value):
    ref[0] = value[0]
    ref[1] = value[1]


def rows_of(ref, start, size):
    start = pl.multiple_of(start, size)
    return ref[0, pl.ds(start, size), :], ref[1, pl.ds(start, size), :]


def call(body, outs, *args, products=1):
    shapes = [jax.ShapeDtypeStruct(shape, F32) for shape in outs]
    return pl.pallas_call(
        body,
        out_shape=shapes,
        in_specs=[pl.BlockSpec(memory_space=pltpu.VMEM)] * len(args),
        out_specs=[pl.BlockSpec(memory_space=pltpu.VMEM)] * len(outs),
        cost_estimate=pl.CostEstimate(
            flops=products * 3 * 8 * 256**3, bytes_accessed=1 << 20, transcendentals=0
        ),
        compiler_params=pltpu.CompilerParams(vmem_limit_bytes=GRANT),
    )(*args)


def side():
    return lax.rem(lax.axis_index("rows"), 2) == 0


def map_kernel(lower, out):
    count = lower.shape[0]
    value = pair(lower, 0)
    for number in range(1, count):
        value = plain(pair(lower, number), value)
    if count % 2:
        value = negative(value)
    put(out, value)


def local_kernel(piece, pivot, lower, upper, ahead, states, bkeep, bsend, gkeep, cmap, late, work):
    count, width = pivot.shape[0], pivot.shape[-1]
    half = bkeep.shape[1]
    mine = jnp.where(side(), 0, half)
    other = half - mine
    last = None
    for number in range(count):
        columns = slice(number * width, (number + 1) * width)
        value = trans((piece[0, :, columns], piece[1, :, columns]), pair(pivot, number))
        if last is not None:
            value = minus(value, trans(last, pair(lower, number)))
        states[number, 0] = value[0]
        states[number, 1] = value[1]
        last = value
    put(bkeep, rows_of(states.at[count - 1], mine, half))
    put(bsend, rows_of(states.at[count - 1], other, half))
    for number in range(count - 2, -1, -1):
        last = minus(pair(states, number), trans(last, pair(upper, number)))
    put(work, last)
    put(gkeep, rows_of(work, mine, half))
    value = rows_of(work, other, half)
    for part in range(2):
        late[part, width:, :] = value[part]
    levels = [negative(pair(lower, 0))]
    for number in range(1, count - 1):
        levels.append(negative(plain(pair(lower, number), levels[-1])))
    if count > 1:
        levels.append(pair(ahead))
    value = levels[-1]
    for number in range(count - 2, -1, -1):
        value = minus(levels[number], plain(pair(upper, number), value))
    for part in range(2):
        late[part, :width, :] = value[part]
    value = pair(upper, count - 1)
    for number in range(count - 2, -1, -1):
        value = plain(pair(upper, number), value)
    if count % 2:
        value = negative(value)
    put(cmap, value)


def part_of(ref, start, size):
    return ref[0, start : start + size, :], ref[1, start : start + size, :]


def join_kernel(mine, theirs, bmine, btheirs, out_b, out_a):
    first = side()
    a_first = pick(first, pair(mine), pair(theirs))
    a_second = pick(first, pair(theirs), pair(mine))
    b_first = pick(first, pair(bmine), pair(btheirs))
    b_second = pick(first, pair(btheirs), pair(bmine))
    put(out_b, plus(trans(b_first, a_second), b_second))
    put(out_a, plain(a_second, a_first))


def join_back_kernel(mine, theirs, out):
    first = side()
    c_first = pick(first, pair(mine), pair(theirs))
    c_second = pick(first, pair(theirs), pair(mine))
    put(out, plain(c_first, c_second))


def apply_kernel(state, matrix, base, out):
    put(out, plus(trans(pair(state), pair(matrix)), pair(base)))


def enter_kernel(inflow, a_mine, a_theirs, b_mine, b_theirs, in_own, in_other):
    first = side()
    entering = pair(inflow)
    a_first = pick(first, pair(a_mine), pair(a_theirs))
    second = plus(trans(entering, a_first), pick(first, pair(b_mine), pair(b_theirs)))
    put(in_own, pick(first, entering, second))
    put(in_other, pick(first, second, entering))


def turn_kernel(in_own, in_other, g_mine, late_mine, late_theirs, c_mine, c_theirs, mid, *outs):
    first = side()
    size = c_mine.shape[1]
    half = in_own.shape[1]
    entering = pick(first, pair(in_own), pair(in_other))
    second = pick(first, pair(in_other), pair(in_own))
    r_mine, r_theirs = part_of(late_mine, 0, size), part_of(late_theirs, 0, size)
    g_own, g_theirs = pair(g_mine), part_of(late_theirs, size, half)
    middle = plus(pick(first, g_theirs, g_own), trans(second, pick(first, r_theirs, r_mine)))
    put(mid, middle)
    value = plus(pick(first, g_own, g_theirs), trans(entering, pick(first, r_mine, r_theirs)))
    value = plus(value, trans(middle, pick(first, pair(c_mine), pair(c_theirs))))
    if len(outs) == 1:
        put(outs[0], value)
        return
    quarter = half // 2
    low = (value[0][:quarter], value[1][:quarter])
    high = (value[0][quarter:], value[1][quarter:])
    source = back_place(4) == 0
    put(outs[0], pick(source, low, high))
    put(outs[1], pick(source, high, low))


def back_place(nodes):
    return nodes - 1 - lax.div(lax.axis_index("rows"), 2)


def middle_kernel(mine_a, mine_b, came_a, came_b, c_mine, c_other, keep, send, last):
    place = back_place(4)
    one = place == 1
    c_one = pick(one, pair(c_mine), pair(c_other))
    c_two = pick(one, pair(c_other), pair(c_mine))
    start = pick(one, pair(came_a), pair(came_b))
    second = plus(trans(start, c_one), pick(one, pair(mine_b), pair(came_a)))
    third = plus(trans(second, c_two), pick(one, pair(came_b), pair(mine_a)))
    put(keep, pick(one, start, second))
    put(send, pick(place == 0, pair(mine_b), pick(one, second, third)))
    put(last, third)


def back_in(entering, mid, c_mine, c_theirs, own, other):
    first = side()
    first_in = plus(pair(mid), trans(entering, pick(first, pair(c_theirs), pair(c_mine))))
    put(own, pick(first, first_in, entering))
    put(other, pick(first, entering, first_in))


def back_in_kernel(back_inflow, *refs):
    back_in(pair(back_inflow), *refs)


def back_in_parts_kernel(keep, came, last, mid, c_mine, c_theirs, own, other, work):
    place = back_place(4)
    low = pick(place == 1, pair(keep), pick(place == 2, pair(came), pair(last)))
    high = pick(place == 2, pair(keep), pair(came))
    quarter = keep.shape[1]
    for part in range(2):
        work[part, :quarter] = low[part]
        work[part, quarter:] = high[part]
    back_in(pair(work), mid, c_mine, c_theirs, own, other)


def swept_kernel(states, in_own, in_theirs, lower, upper, out_own, out_theirs):
    count = states.shape[0]
    half = in_own.shape[1]
    mine = jnp.where(side(), 0, half)
    for carry, start, out in ((in_own, mine, out_own), (in_theirs, half - mine, out_theirs)):
        carry = pair(carry)
        for number in range(count):
            carry = negative(trans(carry, pair(lower, number)))
            put(out.at[number], plus(rows_of(states.at[number], start, half), carry))


def solved_kernel(swept, entering, upper, weights, keep, send):
    count, width = swept.shape[0], swept.shape[-1]
    wreal, wimag = weights[0, 0], weights[0, 1]
    carry = pair(entering)
    upward = lax.rem(lax.axis_index("pole"), 2) == 1
    values = [None] * count
    for number in range(count - 1, -1, -1):
        carry = minus(pair(swept, number), trans(carry, pair(upper, number)))
        values[number] = (
            wreal * carry[0] - wimag * carry[1], wreal * carry[1] + wimag * carry[0]
        )
    blocks = count // 2
    for number in range(blocks):
        columns = slice(number * width, (number + 1) * width)
        for part in range(2):
            low, high = values[number][part], values[number + blocks][part]
            keep[part, :, columns] = jnp.where(upward, high, low)
            send[part, :, columns] = jnp.where(upward, low, high)


def gram_kernel(own, own_more, theirs, theirs_more, total, keep, send, work):
    size = total.shape[1]
    half = size // 2
    mine = jnp.where(side(), 0, half)
    for first, second, start in ((own, own_more, mine), (theirs, theirs_more, half - mine)):
        start = pl.multiple_of(start, half)
        for part in range(2):
            total[part, pl.ds(start, half), :] = first[part] + second[part]
    basis = pair(total)
    dims = ((1,), (1,))
    real = dot(basis[0], basis[0], dims, HIGH) + dot(basis[1], basis[1], dims, HIGH)
    imag = dot(basis[0], basis[1], dims, HIGH) - dot(basis[1], basis[0], dims, HIGH)
    row = lax.broadcasted_iota(jnp.int32, (size, size), 0)
    column = lax.broadcasted_iota(jnp.int32, (size, size), 1)
    work[...] = jnp.where(row <= column, real, imag)
    start = pl.multiple_of(lax.rem(lax.axis_index("pole"), 2) * half, half)
    keep[...] = work[pl.ds(start, half), :]
    send[...] = work[pl.ds(pl.multiple_of(half - start, half), half), :]


def parts_kernel(mine, theirs, high, low):
    for number, piece in enumerate((mine, theirs)):
        for part in range(2):
            high[number, part], low[number, part] = halves(piece[part])


def finish_kernel(states, mine, theirs, q_high, q_low, out, held, slab):
    size = held.shape[0]
    half = size // 2
    columns = out.shape[1]
    pole = lax.axis_index("pole")
    start = pl.multiple_of(lax.rem(pole, 2) * half, half)
    held[pl.ds(start, half), :] = mine[...]
    held[pl.ds(pl.multiple_of(half - start, half), half), :] = theirs[...]
    packed = held[...]
    turned = packed.T
    row = lax.broadcasted_iota(jnp.int32, (size, size), 0)
    column = lax.broadcasted_iota(jnp.int32, (size, size), 1)
    real = jnp.where(row <= column, packed, turned)
    imag = jnp.where(row < column, turned, jnp.where(row > column, -packed, 0.0))
    frob = jnp.sqrt(jnp.sum(real * real + imag * imag, keepdims=True))
    scale = 1.0 / frob
    current = (real * scale, imag * scale)
    put(slab, current)
    factor = (jnp.where(row == column, 1.5, 0.0) - 0.5 * current[0], -0.5 * current[1])
    factor = (halves(factor[0]), halves(factor[1]))
    dims = ((1,), (0,))
    place = pl.multiple_of(pole * columns, columns)
    strip = (slab[0, pl.ds(place, columns), :], slab[1, pl.ds(place, columns), :])
    strip = few(few(strip, factor, dims), factor, dims)
    on = lax.broadcasted_iota(jnp.int32, strip[0].shape, 0) + place
    on = on == lax.broadcasted_iota(jnp.int32, strip[0].shape, 1)
    strip = (jnp.where(on, 1.5, 0.0) - 0.5 * strip[0], -0.5 * strip[1])
    mixing = few(strip, factor, dims)
    factor = jnp.sqrt(states / frob)
    mixing = (mixing[0] * factor, mixing[1] * factor)
    width = q_high.shape[3]
    place = lax.rem(pole, 2) * width
    for number, offset in enumerate((place, width - place)):
        parts = tuple((q_high[number, part], q_low[number, part]) for part in range(2))
        value = few(mixing, parts, dims)
        for part in range(2):
            out[part, :, pl.ds(pl.multiple_of(offset, width), width)] = value[part]


def shards(subspace, pivots, lower_blocks, upper_blocks, pole_weights):
    devices = lax.axis_size("rows")
    poles = lax.axis_size("pole")
    count, width = pivots.shape[1], pivots.shape[-1]
    vectors = subspace.shape[1]
    half = vectors // 2
    nodes = devices // 2
    pivot, lower, upper = pivots[0], lower_blocks[0], upper_blocks[0]
    square = (2, width, width)
    state = (2, vectors, width)
    strip = (2, half, width)
    vmem = pltpu.VMEM

    def scratch(body, outs, extra, *args, products=1):
        return pl.pallas_call(
            body,
            out_shape=[jax.ShapeDtypeStruct(shape, F32) for shape in outs],
            in_specs=[pl.BlockSpec(memory_space=vmem)] * len(args),
            out_specs=[pl.BlockSpec(memory_space=vmem)] * len(outs),
            scratch_shapes=[vmem(shape, F32) for shape in extra],
            cost_estimate=pl.CostEstimate(
                flops=products * 3 * 8 * 256**3, bytes_accessed=1 << 20, transcendentals=0
            ),
            compiler_params=pltpu.CompilerParams(vmem_limit_bytes=GRANT),
        )(*args)

    swap = [(place, place ^ 1) for place in range(devices)]

    def beside(value):
        return lax.ppermute(value, "rows", swap)

    def between(value, moves):
        return lax.ppermute(
            value, "rows", [(2 * a + s, 2 * b + s) for a, b in moves for s in range(2)]
        )

    def prefix(base, matrix, order):
        inflow = None
        for hop in range(nodes - 1):
            passed = base
            if hop:
                (passed,) = call(apply_kernel, [strip], inflow, matrix, base)
            came = between(passed, [(order[hop], order[hop + 1])])
            inflow = came if inflow is None else inflow + came
        return jnp.zeros(strip, F32) if inflow is None else inflow

    (a_mine,) = call(map_kernel, [square], lower)
    a_theirs = beside(a_mine)
    states, b_mine, b_send, g_mine, c_mine, late_mine = scratch(
        local_kernel,
        [(count,) + state, strip, strip, strip, square, (2, width + half, width)],
        [state], subspace, pivot, lower, upper, a_mine, products=2 * count + 3,
    )
    b_theirs = beside(b_send)
    c_theirs = beside(c_mine)
    late_theirs = beside(late_mine)

    b_node, a_node = call(join_kernel, [strip, square], a_mine, a_theirs, b_mine, b_theirs)
    order = list(range(nodes))
    inflow = prefix(b_node, a_node, order)
    (c_node,) = call(join_back_kernel, [square], c_mine, c_theirs)
    quarter = (2, half // 2, width)
    short = nodes == 4
    in_own, in_other = call(enter_kernel, [strip] * 2, inflow, a_mine, a_theirs, b_mine, b_theirs)
    in_theirs = beside(in_other)
    mid, *ends = call(
        turn_kernel, [strip] + ([quarter] * 2 if short else [strip]), in_own, in_other,
        g_mine, late_mine, late_theirs, c_mine, c_theirs, products=2,
    )
    if short:
        c_other = between(c_node, [(1, 2), (2, 1)])
        came_a = between(ends[0], [(3, 2), (2, 1)])
        came_b = between(ends[1], [(3, 1), (1, 2)])
        keep, send, last = call(
            middle_kernel, [quarter] * 3, *ends, came_a, came_b, c_node, c_other
        )
        came = between(send, [(3, 2), (2, 1), (1, 0)])
        last = between(last, [(2, 0)])
    else:
        back_inflow = prefix(ends[0], c_node, order[::-1])
    swept_own, swept_theirs = call(
        swept_kernel, [(count,) + strip] * 2, states, in_own, in_theirs, lower, upper,
        products=count,
    )
    if short:
        x_own, x_other = scratch(
            back_in_parts_kernel, [strip] * 2, [strip], keep, came, last, mid, c_mine, c_theirs
        )
    else:
        x_own, x_other = call(
            back_in_kernel, [strip] * 2, back_inflow, mid, c_mine, c_theirs
        )
    x_theirs = beside(x_other)

    def over_poles(value, bit):
        return lax.ppermute(value, "pole", [(place, place ^ (1 << bit)) for place in range(poles)])

    levels = poles.bit_length() - 1
    columns = count * width
    block = (2, half, columns // 2)

    def poled(swept, entering):
        keep, send = pl.pallas_call(
            solved_kernel,
            out_shape=[jax.ShapeDtypeStruct(block, F32)] * 2,
            in_specs=[pl.BlockSpec(memory_space=vmem)] * 3
            + [pl.BlockSpec(memory_space=pltpu.SMEM)],
            out_specs=[pl.BlockSpec(memory_space=vmem)] * 2,
            compiler_params=pltpu.CompilerParams(vmem_limit_bytes=GRANT),
        )(swept, entering, upper, pole_weights)
        value, more = keep, over_poles(send, 0)
        for bit in range(1, levels):
            value = value + more
            more = over_poles(value, bit)
        return value, more

    own, own_more = poled(swept_own, x_own)
    theirs, theirs_more = poled(swept_theirs, x_theirs)
    total, packed, packed_send = scratch(
        gram_kernel, [(2, vectors, columns // 2), (half, vectors), (half, vectors)],
        [(vectors, vectors)], own, own_more, theirs, theirs_more,
    )
    packed = packed + over_poles(packed_send, 0)
    for bit in range(devices.bit_length() - 1):
        mask = (2 << bit) - 2 if bit else 1
        packed = packed + lax.ppermute(
            packed, "rows", [(place, place ^ mask) for place in range(devices)]
        )
    packed_theirs = over_poles(packed, 0)
    total_theirs = over_poles(total, 0)
    q_high, q_low = pl.pallas_call(
        parts_kernel,
        out_shape=[jax.ShapeDtypeStruct((2,) + total.shape, jnp.bfloat16)] * 2,
        in_specs=[pl.BlockSpec(memory_space=vmem)] * 2,
        out_specs=[pl.BlockSpec(memory_space=vmem)] * 2,
        compiler_params=pltpu.CompilerParams(vmem_limit_bytes=GRANT),
    )(total, total_theirs)
    (result,) = scratch(
        functools.partial(finish_kernel, float(columns * devices)),
        [(2, vectors // poles, columns)], [(vectors, vectors), state],
        packed, packed_theirs, q_high, q_low, products=4,
    )
    return result


def solution(mesh):
    placed = (
        P(None, None, "rows"),
        P("pole", "rows", None, None, None),
        P("pole", "rows", None, None, None),
        P("pole", "rows", None, None, None),
        P("pole", None),
    )
    return jax.shard_map(
        shards, mesh=mesh, in_specs=placed, out_specs=P(None, "pole", "rows"), check_vma=False
    )
```

```python
import functools

import jax
import jax.numpy as jnp
from jax import lax
from jax.experimental import pallas as pl
from jax.experimental.pallas import tpu as pltpu
from jax.sharding import PartitionSpec as P


GRANT = 8 << 20
LANES = 128
HIGH = lax.Precision.HIGH
F32 = jnp.float32


def dot(a, b, dims, precision=None):
    return lax.dot_general(
        a, b, (dims, ((), ())), precision=precision, preferred_element_type=F32
    )


def halves(a):
    high = a.astype(jnp.bfloat16)
    return high, (a - high.astype(F32)).astype(jnp.bfloat16)


def stacked(value):
    real, imag = halves(value[0]), halves(value[1])
    high = jnp.concatenate([real[0], imag[0]], axis=0)
    return high, jnp.concatenate([high, real[1], imag[1]], axis=0)


def against(left, part, dims):
    high, both = left
    size = high.shape[0]
    wide = dot(both, part[0], dims)
    value = wide[:size] + (wide[size:] + dot(high, part[1], dims))
    return value[: size // 2], value[size // 2 :]


def few(left, parts, dims):
    left = stacked(left)
    with_real, with_imag = against(left, parts[0], dims), against(left, parts[1], dims)
    return with_real[0] - with_imag[1], with_imag[0] + with_real[1]


def times(left, right, dims):
    rows = left[0].shape[0]
    if rows <= LANES // 2 or (rows <= LANES and dims[1] == (1,)):
        return few(left, (halves(right[0]), halves(right[1])), dims)
    real = dot(left[0], right[0], dims, HIGH) - dot(left[1], right[1], dims, HIGH)
    imag = dot(left[0], right[1], dims, HIGH) + dot(left[1], right[0], dims, HIGH)
    return real, imag


def plain(left, right):
    return times(left, right, ((1,), (0,)))


def trans(left, right):
    return times(left, right, ((1,), (1,)))


def plus(a, b):
    return a[0] + b[0], a[1] + b[1]


def minus(a, b):
    return a[0] - b[0], a[1] - b[1]


def negative(a):
    return -a[0], -a[1]


def pick(choice, a, b):
    return jnp.where(choice, a[0], b[0]), jnp.where(choice, a[1], b[1])


def pair(ref, *index):
    return ref[(*index, 0)], ref[(*index, 1)]


def put(ref, value):
    ref[0] = value[0]
    ref[1] = value[1]


def rows_of(ref, start, size):
    start = pl.multiple_of(start, size)
    return ref[0, pl.ds(start, size), :], ref[1, pl.ds(start, size), :]


def call(body, outs, *args, products=1):
    shapes = [jax.ShapeDtypeStruct(shape, F32) for shape in outs]
    return pl.pallas_call(
        body,
        out_shape=shapes,
        in_specs=[pl.BlockSpec(memory_space=pltpu.VMEM)] * len(args),
        out_specs=[pl.BlockSpec(memory_space=pltpu.VMEM)] * len(outs),
        cost_estimate=pl.CostEstimate(
            flops=products * 3 * 8 * 256**3, bytes_accessed=1 << 20, transcendentals=0
        ),
        compiler_params=pltpu.CompilerParams(vmem_limit_bytes=GRANT),
    )(*args)


def side():
    return lax.rem(lax.axis_index("rows"), 2) == 0


def map_kernel(lower, out):
    count = lower.shape[0]
    value = pair(lower, 0)
    for number in range(1, count):
        value = plain(pair(lower, number), value)
    if count % 2:
        value = negative(value)
    put(out, value)


def local_kernel(piece, pivot, lower, upper, ahead, states, bkeep, bsend, gkeep, cmap, late, work):
    count, width = pivot.shape[0], pivot.shape[-1]
    half = bkeep.shape[1]
    mine = jnp.where(side(), 0, half)
    other = half - mine
    last = None
    for number in range(count):
        columns = slice(number * width, (number + 1) * width)
        value = trans((piece[0, :, columns], piece[1, :, columns]), pair(pivot, number))
        if last is not None:
            value = minus(value, trans(last, pair(lower, number)))
        states[number, 0] = value[0]
        states[number, 1] = value[1]
        last = value
    put(bkeep, rows_of(states.at[count - 1], mine, half))
    put(bsend, rows_of(states.at[count - 1], other, half))
    for number in range(count - 2, -1, -1):
        last = minus(pair(states, number), trans(last, pair(upper, number)))
    put(work, last)
    put(gkeep, rows_of(work, mine, half))
    value = rows_of(work, other, half)
    for part in range(2):
        late[part, width:, :] = value[part]
    levels = [negative(pair(lower, 0))]
    for number in range(1, count - 1):
        levels.append(negative(plain(pair(lower, number), levels[-1])))
    if count > 1:
        levels.append(pair(ahead))
    value = levels[-1]
    for number in range(count - 2, -1, -1):
        value = minus(levels[number], plain(pair(upper, number), value))
    for part in range(2):
        late[part, :width, :] = value[part]
    value = pair(upper, count - 1)
    for number in range(count - 2, -1, -1):
        value = plain(pair(upper, number), value)
    if count % 2:
        value = negative(value)
    put(cmap, value)


def part_of(ref, start, size):
    return ref[0, start : start + size, :], ref[1, start : start + size, :]


def join_kernel(mine, theirs, bmine, btheirs, out_b, out_a):
    first = side()
    a_first = pick(first, pair(mine), pair(theirs))
    a_second = pick(first, pair(theirs), pair(mine))
    b_first = pick(first, pair(bmine), pair(btheirs))
    b_second = pick(first, pair(btheirs), pair(bmine))
    put(out_b, plus(trans(b_first, a_second), b_second))
    put(out_a, plain(a_second, a_first))


def join_back_kernel(mine, theirs, out):
    first = side()
    c_first = pick(first, pair(mine), pair(theirs))
    c_second = pick(first, pair(theirs), pair(mine))
    put(out, plain(c_first, c_second))


def apply_kernel(state, matrix, base, out):
    put(out, plus(trans(pair(state), pair(matrix)), pair(base)))


def enter_kernel(inflow, a_mine, a_theirs, b_mine, b_theirs, in_own, in_other):
    first = side()
    entering = pair(inflow)
    a_first = pick(first, pair(a_mine), pair(a_theirs))
    second = plus(trans(entering, a_first), pick(first, pair(b_mine), pair(b_theirs)))
    put(in_own, pick(first, entering, second))
    put(in_other, pick(first, second, entering))


def turn_kernel(in_own, in_other, g_mine, late_mine, late_theirs, c_mine, c_theirs, mid, *outs):
    first = side()
    size = c_mine.shape[1]
    half = in_own.shape[1]
    entering = pick(first, pair(in_own), pair(in_other))
    second = pick(first, pair(in_other), pair(in_own))
    r_mine, r_theirs = part_of(late_mine, 0, size), part_of(late_theirs, 0, size)
    g_own, g_theirs = pair(g_mine), part_of(late_theirs, size, half)
    middle = plus(pick(first, g_theirs, g_own), trans(second, pick(first, r_theirs, r_mine)))
    put(mid, middle)
    value = plus(pick(first, g_own, g_theirs), trans(entering, pick(first, r_mine, r_theirs)))
    value = plus(value, trans(middle, pick(first, pair(c_mine), pair(c_theirs))))
    if len(outs) == 1:
        put(outs[0], value)
        return
    quarter = half // 2
    low = (value[0][:quarter], value[1][:quarter])
    high = (value[0][quarter:], value[1][quarter:])
    source = back_place(4) == 0
    put(outs[0], pick(source, low, high))
    put(outs[1], pick(source, high, low))


def back_place(nodes):
    return nodes - 1 - lax.div(lax.axis_index("rows"), 2)


def middle_kernel(mine_a, mine_b, came_a, came_b, c_mine, c_other, keep, send, last):
    place = back_place(4)
    one = place == 1
    c_one = pick(one, pair(c_mine), pair(c_other))
    c_two = pick(one, pair(c_other), pair(c_mine))
    start = pick(one, pair(came_a), pair(came_b))
    second = plus(trans(start, c_one), pick(one, pair(mine_b), pair(came_a)))
    third = plus(trans(second, c_two), pick(one, pair(came_b), pair(mine_a)))
    put(keep, pick(one, start, second))
    put(send, pick(place == 0, pair(mine_b), pick(one, second, third)))
    put(last, third)


def back_in(entering, mid, c_mine, c_theirs, own, other):
    first = side()
    first_in = plus(pair(mid), trans(entering, pick(first, pair(c_theirs), pair(c_mine))))
    put(own, pick(first, first_in, entering))
    put(other, pick(first, entering, first_in))


def back_in_kernel(back_inflow, *refs):
    back_in(pair(back_inflow), *refs)


def back_in_parts_kernel(keep, came, last, mid, c_mine, c_theirs, own, other, work):
    place = back_place(4)
    low = pick(place == 1, pair(keep), pick(place == 2, pair(came), pair(last)))
    high = pick(place == 2, pair(keep), pair(came))
    quarter = keep.shape[1]
    for part in range(2):
        work[part, :quarter] = low[part]
        work[part, quarter:] = high[part]
    back_in(pair(work), mid, c_mine, c_theirs, own, other)


def swept_kernel(states, in_own, in_theirs, lower, upper, weights, out_own, out_theirs):
    count = states.shape[0]
    half = in_own.shape[1]
    mine = jnp.where(side(), 0, half)
    for carry, start, out in ((in_own, mine, out_own), (in_theirs, half - mine, out_theirs)):
        carry = pair(carry)
        for number in range(count):
            carry = negative(trans(carry, pair(lower, number)))
            put(out.at[number], plus(rows_of(states.at[number], start, half), carry))


def solved_kernel(swept, entering, upper, weights, keep, send):
    count, width = swept.shape[0], swept.shape[-1]
    wreal, wimag = weights[0, 0], weights[0, 1]
    carry = pair(entering)
    upward = lax.rem(lax.axis_index("pole"), 2) == 1
    values = [None] * count
    for number in range(count - 1, -1, -1):
        carry = minus(pair(swept, number), trans(carry, pair(upper, number)))
        values[number] = (
            wreal * carry[0] - wimag * carry[1], wreal * carry[1] + wimag * carry[0]
        )
    blocks = count // 2
    for number in range(blocks):
        columns = slice(number * width, (number + 1) * width)
        for part in range(2):
            low, high = values[number][part], values[number + blocks][part]
            keep[part, :, columns] = jnp.where(upward, high, low)
            send[part, :, columns] = jnp.where(upward, low, high)


def gram_kernel(own, own_more, theirs, theirs_more, total, keep, send, work):
    size = total.shape[1]
    half = size // 2
    mine = jnp.where(side(), 0, half)
    for first, second, start in ((own, own_more, mine), (theirs, theirs_more, half - mine)):
        start = pl.multiple_of(start, half)
        for part in range(2):
            total[part, pl.ds(start, half), :] = first[part] + second[part]
    basis = pair(total)
    dims = ((1,), (1,))
    real = dot(basis[0], basis[0], dims, HIGH) + dot(basis[1], basis[1], dims, HIGH)
    imag = dot(basis[0], basis[1], dims, HIGH) - dot(basis[1], basis[0], dims, HIGH)
    row = lax.broadcasted_iota(jnp.int32, (size, size), 0)
    column = lax.broadcasted_iota(jnp.int32, (size, size), 1)
    work[...] = jnp.where(row <= column, real, imag)
    start = pl.multiple_of(lax.rem(lax.axis_index("pole"), 2) * half, half)
    keep[...] = work[pl.ds(start, half), :]
    send[...] = work[pl.ds(pl.multiple_of(half - start, half), half), :]


def parts_kernel(mine, theirs, high, low):
    for number, piece in enumerate((mine, theirs)):
        for part in range(2):
            high[number, part], low[number, part] = halves(piece[part])


def finish_kernel(states, mine, theirs, q_high, q_low, out, held, slab):
    size = held.shape[0]
    half = size // 2
    columns = out.shape[1]
    pole = lax.axis_index("pole")
    start = pl.multiple_of(lax.rem(pole, 2) * half, half)
    held[pl.ds(start, half), :] = mine[...]
    held[pl.ds(pl.multiple_of(half - start, half), half), :] = theirs[...]
    packed = held[...]
    turned = packed.T
    row = lax.broadcasted_iota(jnp.int32, (size, size), 0)
    column = lax.broadcasted_iota(jnp.int32, (size, size), 1)
    real = jnp.where(row <= column, packed, turned)
    imag = jnp.where(row < column, turned, jnp.where(row > column, -packed, 0.0))
    frob = jnp.sqrt(jnp.sum(real * real + imag * imag, keepdims=True))
    scale = 1.0 / frob
    current = (real * scale, imag * scale)
    put(slab, current)
    factor = (jnp.where(row == column, 1.5, 0.0) - 0.5 * current[0], -0.5 * current[1])
    factor = (halves(factor[0]), halves(factor[1]))
    dims = ((1,), (0,))
    place = pl.multiple_of(pole * columns, columns)
    strip = (slab[0, pl.ds(place, columns), :], slab[1, pl.ds(place, columns), :])
    strip = few(few(strip, factor, dims), factor, dims)
    on = lax.broadcasted_iota(jnp.int32, strip[0].shape, 0) + place
    on = on == lax.broadcasted_iota(jnp.int32, strip[0].shape, 1)
    strip = (jnp.where(on, 1.5, 0.0) - 0.5 * strip[0], -0.5 * strip[1])
    mixing = few(strip, factor, dims)
    factor = jnp.sqrt(states / frob)
    mixing = (mixing[0] * factor, mixing[1] * factor)
    width = q_high.shape[3]
    place = lax.rem(pole, 2) * width
    for number, offset in enumerate((place, width - place)):
        parts = tuple((q_high[number, part], q_low[number, part]) for part in range(2))
        value = few(mixing, parts, dims)
        for part in range(2):
            out[part, :, pl.ds(pl.multiple_of(offset, width), width)] = value[part]


def shards(subspace, pivots, lower_blocks, upper_blocks, pole_weights):
    devices = lax.axis_size("rows")
    poles = lax.axis_size("pole")
    count, width = pivots.shape[1], pivots.shape[-1]
    vectors = subspace.shape[1]
    half = vectors // 2
    nodes = devices // 2
    pivot, lower, upper = pivots[0], lower_blocks[0], upper_blocks[0]
    square = (2, width, width)
    state = (2, vectors, width)
    strip = (2, half, width)
    vmem = pltpu.VMEM

    def scratch(body, outs, extra, *args, products=1):
        return pl.pallas_call(
            body,
            out_shape=[jax.ShapeDtypeStruct(shape, F32) for shape in outs],
            in_specs=[pl.BlockSpec(memory_space=vmem)] * len(args),
            out_specs=[pl.BlockSpec(memory_space=vmem)] * len(outs),
            scratch_shapes=[vmem(shape, F32) for shape in extra],
            cost_estimate=pl.CostEstimate(
                flops=products * 3 * 8 * 256**3, bytes_accessed=1 << 20, transcendentals=0
            ),
            compiler_params=pltpu.CompilerParams(vmem_limit_bytes=GRANT),
        )(*args)

    swap = [(place, place ^ 1) for place in range(devices)]

    def beside(value):
        return lax.ppermute(value, "rows", swap)

    def between(value, moves):
        return lax.ppermute(
            value, "rows", [(2 * a + s, 2 * b + s) for a, b in moves for s in range(2)]
        )

    def prefix(base, matrix, order):
        inflow = None
        for hop in range(nodes - 1):
            passed = base
            if hop:
                (passed,) = call(apply_kernel, [strip], inflow, matrix, base)
            came = between(passed, [(order[hop], order[hop + 1])])
            inflow = came if inflow is None else inflow + came
        return jnp.zeros(strip, F32) if inflow is None else inflow

    (a_mine,) = call(map_kernel, [square], lower)
    a_theirs = beside(a_mine)
    states, b_mine, b_send, g_mine, c_mine, late_mine = scratch(
        local_kernel,
        [(count,) + state, strip, strip, strip, square, (2, width + half, width)],
        [state], subspace, pivot, lower, upper, a_mine, products=2 * count + 3,
    )
    b_theirs = beside(b_send)
    c_theirs = beside(c_mine)
    late_theirs = beside(late_mine)

    b_node, a_node = call(join_kernel, [strip, square], a_mine, a_theirs, b_mine, b_theirs)
    order = list(range(nodes))
    inflow = prefix(b_node, a_node, order)
    (c_node,) = call(join_back_kernel, [square], c_mine, c_theirs)
    quarter = (2, half // 2, width)
    short = nodes == 4
    in_own, in_other = call(enter_kernel, [strip] * 2, inflow, a_mine, a_theirs, b_mine, b_theirs)
    in_theirs = beside(in_other)
    mid, *ends = call(
        turn_kernel, [strip] + ([quarter] * 2 if short else [strip]), in_own, in_other,
        g_mine, late_mine, late_theirs, c_mine, c_theirs, products=2,
    )
    if short:
        c_other = between(c_node, [(1, 2), (2, 1)])
        came_a = between(ends[0], [(3, 2), (2, 1)])
        came_b = between(ends[1], [(3, 1), (1, 2)])
        keep, send, last = call(
            middle_kernel, [quarter] * 3, *ends, came_a, came_b, c_node, c_other
        )
        came = between(send, [(3, 2), (2, 1), (1, 0)])
        last = between(last, [(2, 0)])
    else:
        back_inflow = prefix(ends[0], c_node, order[::-1])
    swept_own, swept_theirs = pl.pallas_call(
        swept_kernel,
        out_shape=[jax.ShapeDtypeStruct((count,) + strip, F32)] * 2,
        in_specs=[pl.BlockSpec(memory_space=vmem)] * 5
        + [pl.BlockSpec(memory_space=pltpu.SMEM)],
        out_specs=[pl.BlockSpec(memory_space=vmem)] * 2,
        compiler_params=pltpu.CompilerParams(vmem_limit_bytes=GRANT),
    )(states, in_own, in_theirs, lower, upper, pole_weights)
    if short:
        x_own, x_other = scratch(
            back_in_parts_kernel, [strip] * 2, [strip], keep, came, last, mid, c_mine, c_theirs
        )
    else:
        x_own, x_other = call(
            back_in_kernel, [strip] * 2, back_inflow, mid, c_mine, c_theirs
        )
    x_theirs = beside(x_other)

    def over_poles(value, bit):
        return lax.ppermute(value, "pole", [(place, place ^ (1 << bit)) for place in range(poles)])

    levels = poles.bit_length() - 1
    columns = count * width
    block = (2, half, columns // 2)

    def poled(swept, entering):
        keep, send = pl.pallas_call(
            solved_kernel,
            out_shape=[jax.ShapeDtypeStruct(block, F32)] * 2,
            in_specs=[pl.BlockSpec(memory_space=vmem)] * 3
            + [pl.BlockSpec(memory_space=pltpu.SMEM)],
            out_specs=[pl.BlockSpec(memory_space=vmem)] * 2,
            compiler_params=pltpu.CompilerParams(vmem_limit_bytes=GRANT),
        )(swept, entering, upper, pole_weights)
        value, more = keep, over_poles(send, 0)
        for bit in range(1, levels):
            value = value + more
            more = over_poles(value, bit)
        return value, more

    own, own_more = poled(swept_own, x_own)
    theirs, theirs_more = poled(swept_theirs, x_theirs)
    total, packed, packed_send = scratch(
        gram_kernel, [(2, vectors, columns // 2), (half, vectors), (half, vectors)],
        [(vectors, vectors)], own, own_more, theirs, theirs_more,
    )
    packed = packed + over_poles(packed_send, 0)
    for bit in range(devices.bit_length() - 1):
        mask = (2 << bit) - 2 if bit else 1
        packed = packed + lax.ppermute(
            packed, "rows", [(place, place ^ mask) for place in range(devices)]
        )
    packed_theirs = over_poles(packed, 0)
    total_theirs = over_poles(total, 0)
    q_high, q_low = pl.pallas_call(
        parts_kernel,
        out_shape=[jax.ShapeDtypeStruct((2,) + total.shape, jnp.bfloat16)] * 2,
        in_specs=[pl.BlockSpec(memory_space=vmem)] * 2,
        out_specs=[pl.BlockSpec(memory_space=vmem)] * 2,
        compiler_params=pltpu.CompilerParams(vmem_limit_bytes=GRANT),
    )(total, total_theirs)
    (result,) = scratch(
        functools.partial(finish_kernel, float(columns * devices)),
        [(2, vectors // poles, columns)], [(vectors, vectors), state],
        packed, packed_theirs, q_high, q_low, products=4,
    )
    return result


def solution(mesh):
    placed = (
        P(None, None, "rows"),
        P("pole", "rows", None, None, None),
        P("pole", "rows", None, None, None),
        P("pole", "rows", None, None, None),
        P("pole", None),
    )
    return jax.shard_map(
        shards, mesh=mesh, in_specs=placed, out_specs=P(None, "pole", "rows"), check_vma=False
    )
```

```python
import functools

import jax
import jax.numpy as jnp
from jax import lax
from jax.experimental import pallas as pl
from jax.experimental.pallas import tpu as pltpu
from jax.sharding import PartitionSpec as P


GRANT = 8 << 20
LANES = 128
HIGH = lax.Precision.HIGH
F32 = jnp.float32


def dot(a, b, dims, precision=None):
    return lax.dot_general(
        a, b, (dims, ((), ())), precision=precision, preferred_element_type=F32
    )


def halves(a):
    high = a.astype(jnp.bfloat16)
    return high, (a - high.astype(F32)).astype(jnp.bfloat16)


def stacked(value):
    real, imag = halves(value[0]), halves(value[1])
    high = jnp.concatenate([real[0], imag[0]], axis=0)
    return high, jnp.concatenate([high, real[1], imag[1]], axis=0)


def against(left, part, dims):
    high, both = left
    size = high.shape[0]
    wide = dot(both, part[0], dims)
    value = wide[:size] + (wide[size:] + dot(high, part[1], dims))
    return value[: size // 2], value[size // 2 :]


def few(left, parts, dims):
    return few_stacked(stacked(left), parts, dims)


def few_stacked(left, parts, dims):
    with_real, with_imag = against(left, parts[0], dims), against(left, parts[1], dims)
    return with_real[0] - with_imag[1], with_imag[0] + with_real[1]


def times(left, right, dims):
    rows = left[0].shape[0]
    if rows <= LANES // 2 or (rows <= LANES and dims[1] == (1,)):
        return few(left, (halves(right[0]), halves(right[1])), dims)
    real = dot(left[0], right[0], dims, HIGH) - dot(left[1], right[1], dims, HIGH)
    imag = dot(left[0], right[1], dims, HIGH) + dot(left[1], right[0], dims, HIGH)
    return real, imag


def plain(left, right):
    return times(left, right, ((1,), (0,)))


def trans(left, right):
    return times(left, right, ((1,), (1,)))


def plus(a, b):
    return a[0] + b[0], a[1] + b[1]


def minus(a, b):
    return a[0] - b[0], a[1] - b[1]


def negative(a):
    return -a[0], -a[1]


def pick(choice, a, b):
    return jnp.where(choice, a[0], b[0]), jnp.where(choice, a[1], b[1])


def pair(ref, *index):
    return ref[(*index, 0)], ref[(*index, 1)]


def put(ref, value):
    ref[0] = value[0]
    ref[1] = value[1]


def rows_of(ref, start, size):
    start = pl.multiple_of(start, size)
    return ref[0, pl.ds(start, size), :], ref[1, pl.ds(start, size), :]


def call(body, outs, *args, products=1):
    shapes = [jax.ShapeDtypeStruct(shape, F32) for shape in outs]
    return pl.pallas_call(
        body,
        out_shape=shapes,
        in_specs=[pl.BlockSpec(memory_space=pltpu.VMEM)] * len(args),
        out_specs=[pl.BlockSpec(memory_space=pltpu.VMEM)] * len(outs),
        cost_estimate=pl.CostEstimate(
            flops=products * 3 * 8 * 256**3, bytes_accessed=1 << 20, transcendentals=0
        ),
        compiler_params=pltpu.CompilerParams(vmem_limit_bytes=GRANT),
    )(*args)


def side():
    return lax.rem(lax.axis_index("rows"), 2) == 0


def map_kernel(lower, out):
    count = lower.shape[0]
    value = pair(lower, 0)
    for number in range(1, count):
        value = plain(pair(lower, number), value)
    if count % 2:
        value = negative(value)
    put(out, value)


def local_kernel(piece, pivot, lower, upper, ahead, states, bkeep, bsend, gkeep, cmap, cmaps, late, work):
    count, width = pivot.shape[0], pivot.shape[-1]
    half = bkeep.shape[1]
    mine = jnp.where(side(), 0, half)
    other = half - mine
    last = None
    for number in range(count):
        columns = slice(number * width, (number + 1) * width)
        value = trans((piece[0, :, columns], piece[1, :, columns]), pair(pivot, number))
        if last is not None:
            value = minus(value, trans(last, pair(lower, number)))
        states[number, 0] = value[0]
        states[number, 1] = value[1]
        last = value
    put(bkeep, rows_of(states.at[count - 1], mine, half))
    put(bsend, rows_of(states.at[count - 1], other, half))
    for number in range(count - 2, -1, -1):
        last = minus(pair(states, number), trans(last, pair(upper, number)))
    put(work, last)
    put(gkeep, rows_of(work, mine, half))
    value = rows_of(work, other, half)
    for part in range(2):
        late[part, width:, :] = value[part]
    levels = [negative(pair(lower, 0))]
    for number in range(1, count - 1):
        levels.append(negative(plain(pair(lower, number), levels[-1])))
    if count > 1:
        levels.append(pair(ahead))
    value = levels[-1]
    for number in range(count - 2, -1, -1):
        value = minus(levels[number], plain(pair(upper, number), value))
    for part in range(2):
        late[part, :width, :] = value[part]
    value = negative(pair(upper, count - 1))
    put(cmaps.at[count - 1], value)
    for number in range(count - 2, -1, -1):
        value = negative(plain(pair(upper, number), value))
        put(cmaps.at[number], value)
    put(cmap, value)


def part_of(ref, start, size):
    return ref[0, start : start + size, :], ref[1, start : start + size, :]


def join_kernel(mine, theirs, bmine, btheirs, out_b, out_a):
    first = side()
    a_first = pick(first, pair(mine), pair(theirs))
    a_second = pick(first, pair(theirs), pair(mine))
    b_first = pick(first, pair(bmine), pair(btheirs))
    b_second = pick(first, pair(btheirs), pair(bmine))
    put(out_b, plus(trans(b_first, a_second), b_second))
    put(out_a, plain(a_second, a_first))


def join_back_kernel(mine, theirs, out):
    first = side()
    c_first = pick(first, pair(mine), pair(theirs))
    c_second = pick(first, pair(theirs), pair(mine))
    put(out, plain(c_first, c_second))


def apply_kernel(state, matrix, base, out):
    put(out, plus(trans(pair(state), pair(matrix)), pair(base)))


def enter_kernel(inflow, a_mine, a_theirs, b_mine, b_theirs, in_own, in_other):
    first = side()
    entering = pair(inflow)
    a_first = pick(first, pair(a_mine), pair(a_theirs))
    second = plus(trans(entering, a_first), pick(first, pair(b_mine), pair(b_theirs)))
    put(in_own, pick(first, entering, second))
    put(in_other, pick(first, second, entering))


def turn_kernel(in_own, in_other, g_mine, late_mine, late_theirs, c_mine, c_theirs, mid, *outs):
    first = side()
    size = c_mine.shape[1]
    half = in_own.shape[1]
    entering = pick(first, pair(in_own), pair(in_other))
    second = pick(first, pair(in_other), pair(in_own))
    r_mine, r_theirs = part_of(late_mine, 0, size), part_of(late_theirs, 0, size)
    g_own, g_theirs = pair(g_mine), part_of(late_theirs, size, half)
    middle = plus(pick(first, g_theirs, g_own), trans(second, pick(first, r_theirs, r_mine)))
    put(mid, middle)
    value = plus(pick(first, g_own, g_theirs), trans(entering, pick(first, r_mine, r_theirs)))
    value = plus(value, trans(middle, pick(first, pair(c_mine), pair(c_theirs))))
    if len(outs) == 1:
        put(outs[0], value)
        return
    quarter = half // 2
    low = (value[0][:quarter], value[1][:quarter])
    high = (value[0][quarter:], value[1][quarter:])
    source = back_place(4) == 0
    put(outs[0], pick(source, low, high))
    put(outs[1], pick(source, high, low))


def back_place(nodes):
    return nodes - 1 - lax.div(lax.axis_index("rows"), 2)


def middle_kernel(mine_a, mine_b, came_a, came_b, c_mine, c_other, keep, send, last):
    place = back_place(4)
    one = place == 1
    c_one = pick(one, pair(c_mine), pair(c_other))
    c_two = pick(one, pair(c_other), pair(c_mine))
    start = pick(one, pair(came_a), pair(came_b))
    second = plus(trans(start, c_one), pick(one, pair(mine_b), pair(came_a)))
    third = plus(trans(second, c_two), pick(one, pair(came_b), pair(mine_a)))
    put(keep, pick(one, start, second))
    put(send, pick(place == 0, pair(mine_b), pick(one, second, third)))
    put(last, third)


def back_in(entering, mid, c_mine, c_theirs, own, other):
    first = side()
    first_in = plus(pair(mid), trans(entering, pick(first, pair(c_theirs), pair(c_mine))))
    put(own, pick(first, first_in, entering))
    put(other, pick(first, entering, first_in))


def back_in_kernel(back_inflow, *refs):
    back_in(pair(back_inflow), *refs)


def back_in_parts_kernel(keep, came, last, mid, c_mine, c_theirs, own, other, work):
    place = back_place(4)
    low = pick(place == 1, pair(keep), pick(place == 2, pair(came), pair(last)))
    high = pick(place == 2, pair(keep), pair(came))
    quarter = keep.shape[1]
    for part in range(2):
        work[part, :quarter] = low[part]
        work[part, quarter:] = high[part]
    back_in(pair(work), mid, c_mine, c_theirs, own, other)


def swept_kernel(states, in_own, in_theirs, lower, upper, c_maps, weights, out_own, out_theirs,
                 high, low):
    count = states.shape[0]
    half = in_own.shape[1]
    mine = jnp.where(side(), 0, half)
    for carry, start, out in ((in_own, mine, out_own), (in_theirs, half - mine, out_theirs)):
        carry = pair(carry)
        for number in range(count):
            carry = negative(trans(carry, pair(lower, number)))
            value = plus(rows_of(states.at[number], start, half), carry)
            put(out.at[number], value)
        for number in range(count - 2, -1, -1):
            value = minus(pair(out, number), trans(value, pair(upper, number)))
            put(out.at[number], value)
    for number in range(count):
        for part in range(2):
            high[number, part], low[number, part] = halves(c_maps[number, part])


def solved_kernel(swept, entering, high, low, weights, keep, send):
    count, width = swept.shape[0], swept.shape[-1]
    wreal, wimag = weights[0, 0], weights[0, 1]
    left = stacked(pair(entering))
    upward = lax.rem(lax.axis_index("pole"), 2) == 1
    values = []
    for number in range(count):
        parts = tuple((high[number, part], low[number, part]) for part in range(2))
        product = few_stacked(left, parts, ((1,), (1,)))
        value = plus(pair(swept, number), product)
        values.append((wreal * value[0] - wimag * value[1], wreal * value[1] + wimag * value[0]))
    blocks = count // 2
    for number in range(blocks):
        columns = slice(number * width, (number + 1) * width)
        for part in range(2):
            low, high = values[number][part], values[number + blocks][part]
            keep[part, :, columns] = jnp.where(upward, high, low)
            send[part, :, columns] = jnp.where(upward, low, high)


def gram_kernel(own, own_more, theirs, theirs_more, total, keep, send, work):
    size = total.shape[1]
    half = size // 2
    mine = jnp.where(side(), 0, half)
    for first, second, start in ((own, own_more, mine), (theirs, theirs_more, half - mine)):
        start = pl.multiple_of(start, half)
        for part in range(2):
            total[part, pl.ds(start, half), :] = first[part] + second[part]
    basis = pair(total)
    dims = ((1,), (1,))
    real = dot(basis[0], basis[0], dims, HIGH) + dot(basis[1], basis[1], dims, HIGH)
    imag = dot(basis[0], basis[1], dims, HIGH) - dot(basis[1], basis[0], dims, HIGH)
    row = lax.broadcasted_iota(jnp.int32, (size, size), 0)
    column = lax.broadcasted_iota(jnp.int32, (size, size), 1)
    work[...] = jnp.where(row <= column, real, imag)
    start = pl.multiple_of(lax.rem(lax.axis_index("pole"), 2) * half, half)
    keep[...] = work[pl.ds(start, half), :]
    send[...] = work[pl.ds(pl.multiple_of(half - start, half), half), :]


def parts_kernel(mine, theirs, high, low):
    for number, piece in enumerate((mine, theirs)):
        for part in range(2):
            high[number, part], low[number, part] = halves(piece[part])


def finish_kernel(states, mine, theirs, q_high, q_low, out, held, slab):
    size = held.shape[0]
    half = size // 2
    columns = out.shape[1]
    pole = lax.axis_index("pole")
    start = pl.multiple_of(lax.rem(pole, 2) * half, half)
    held[pl.ds(start, half), :] = mine[...]
    held[pl.ds(pl.multiple_of(half - start, half), half), :] = theirs[...]
    packed = held[...]
    turned = packed.T
    row = lax.broadcasted_iota(jnp.int32, (size, size), 0)
    column = lax.broadcasted_iota(jnp.int32, (size, size), 1)
    real = jnp.where(row <= column, packed, turned)
    imag = jnp.where(row < column, turned, jnp.where(row > column, -packed, 0.0))
    frob = jnp.sqrt(jnp.sum(real * real + imag * imag, keepdims=True))
    scale = 1.0 / frob
    current = (real * scale, imag * scale)
    put(slab, current)
    factor = (jnp.where(row == column, 1.5, 0.0) - 0.5 * current[0], -0.5 * current[1])
    factor = (halves(factor[0]), halves(factor[1]))
    dims = ((1,), (0,))
    place = pl.multiple_of(pole * columns, columns)
    strip = (slab[0, pl.ds(place, columns), :], slab[1, pl.ds(place, columns), :])
    strip = few(few(strip, factor, dims), factor, dims)
    on = lax.broadcasted_iota(jnp.int32, strip[0].shape, 0) + place
    on = on == lax.broadcasted_iota(jnp.int32, strip[0].shape, 1)
    strip = (jnp.where(on, 1.5, 0.0) - 0.5 * strip[0], -0.5 * strip[1])
    mixing = few(strip, factor, dims)
    factor = jnp.sqrt(states / frob)
    mixing = (mixing[0] * factor, mixing[1] * factor)
    width = q_high.shape[3]
    place = lax.rem(pole, 2) * width
    for number, offset in enumerate((place, width - place)):
        parts = tuple((q_high[number, part], q_low[number, part]) for part in range(2))
        value = few(mixing, parts, dims)
        for part in range(2):
            out[part, :, pl.ds(pl.multiple_of(offset, width), width)] = value[part]


def shards(subspace, pivots, lower_blocks, upper_blocks, pole_weights):
    devices = lax.axis_size("rows")
    poles = lax.axis_size("pole")
    count, width = pivots.shape[1], pivots.shape[-1]
    vectors = subspace.shape[1]
    half = vectors // 2
    nodes = devices // 2
    pivot, lower, upper = pivots[0], lower_blocks[0], upper_blocks[0]
    square = (2, width, width)
    state = (2, vectors, width)
    strip = (2, half, width)
    vmem = pltpu.VMEM

    def scratch(body, outs, extra, *args, products=1):
        return pl.pallas_call(
            body,
            out_shape=[jax.ShapeDtypeStruct(shape, F32) for shape in outs],
            in_specs=[pl.BlockSpec(memory_space=vmem)] * len(args),
            out_specs=[pl.BlockSpec(memory_space=vmem)] * len(outs),
            scratch_shapes=[vmem(shape, F32) for shape in extra],
            cost_estimate=pl.CostEstimate(
                flops=products * 3 * 8 * 256**3, bytes_accessed=1 << 20, transcendentals=0
            ),
            compiler_params=pltpu.CompilerParams(vmem_limit_bytes=GRANT),
        )(*args)

    swap = [(place, place ^ 1) for place in range(devices)]

    def beside(value):
        return lax.ppermute(value, "rows", swap)

    def between(value, moves):
        return lax.ppermute(
            value, "rows", [(2 * a + s, 2 * b + s) for a, b in moves for s in range(2)]
        )

    def prefix(base, matrix, order):
        inflow = None
        for hop in range(nodes - 1):
            passed = base
            if hop:
                (passed,) = call(apply_kernel, [strip], inflow, matrix, base)
            came = between(passed, [(order[hop], order[hop + 1])])
            inflow = came if inflow is None else inflow + came
        return jnp.zeros(strip, F32) if inflow is None else inflow

    (a_mine,) = call(map_kernel, [square], lower)
    a_theirs = beside(a_mine)
    states, b_mine, b_send, g_mine, c_mine, c_maps, late_mine = scratch(
        local_kernel,
        [(count,) + state, strip, strip, strip, square, (count,) + square,
         (2, width + half, width)],
        [state], subspace, pivot, lower, upper, a_mine, products=2 * count + 3,
    )
    b_theirs = beside(b_send)
    c_theirs = beside(c_mine)
    late_theirs = beside(late_mine)

    b_node, a_node = call(join_kernel, [strip, square], a_mine, a_theirs, b_mine, b_theirs)
    order = list(range(nodes))
    inflow = prefix(b_node, a_node, order)
    (c_node,) = call(join_back_kernel, [square], c_mine, c_theirs)
    quarter = (2, half // 2, width)
    short = nodes == 4
    in_own, in_other = call(enter_kernel, [strip] * 2, inflow, a_mine, a_theirs, b_mine, b_theirs)
    in_theirs = beside(in_other)
    mid, *ends = call(
        turn_kernel, [strip] + ([quarter] * 2 if short else [strip]), in_own, in_other,
        g_mine, late_mine, late_theirs, c_mine, c_theirs, products=2,
    )
    if short:
        c_other = between(c_node, [(1, 2), (2, 1)])
        came_a = between(ends[0], [(3, 2), (2, 1)])
        came_b = between(ends[1], [(3, 1), (1, 2)])
        keep, send, last = call(
            middle_kernel, [quarter] * 3, *ends, came_a, came_b, c_node, c_other
        )
        came = between(send, [(3, 2), (2, 1), (1, 0)])
        last = between(last, [(2, 0)])
    else:
        back_inflow = prefix(ends[0], c_node, order[::-1])
    swept_own, swept_theirs, c_high, c_low = pl.pallas_call(
        swept_kernel,
        out_shape=[jax.ShapeDtypeStruct((count,) + strip, F32)] * 2
        + [jax.ShapeDtypeStruct((count,) + square, jnp.bfloat16)] * 2,
        in_specs=[pl.BlockSpec(memory_space=vmem)] * 6
        + [pl.BlockSpec(memory_space=pltpu.SMEM)],
        out_specs=[pl.BlockSpec(memory_space=vmem)] * 4,
        compiler_params=pltpu.CompilerParams(vmem_limit_bytes=GRANT),
    )(states, in_own, in_theirs, lower, upper, c_maps, pole_weights)
    if short:
        x_own, x_other = scratch(
            back_in_parts_kernel, [strip] * 2, [strip], keep, came, last, mid, c_mine, c_theirs
        )
    else:
        x_own, x_other = call(
            back_in_kernel, [strip] * 2, back_inflow, mid, c_mine, c_theirs
        )
    x_theirs = beside(x_other)

    def over_poles(value, bit):
        return lax.ppermute(value, "pole", [(place, place ^ (1 << bit)) for place in range(poles)])

    levels = poles.bit_length() - 1
    columns = count * width
    block = (2, half, columns // 2)

    def poled(swept, entering):
        keep, send = pl.pallas_call(
            solved_kernel,
            out_shape=[jax.ShapeDtypeStruct(block, F32)] * 2,
            in_specs=[pl.BlockSpec(memory_space=vmem)] * 4
            + [pl.BlockSpec(memory_space=pltpu.SMEM)],
            out_specs=[pl.BlockSpec(memory_space=vmem)] * 2,
            compiler_params=pltpu.CompilerParams(vmem_limit_bytes=GRANT),
        )(swept, entering, c_high, c_low, pole_weights)
        value, more = keep, over_poles(send, 0)
        for bit in range(1, levels):
            value = value + more
            more = over_poles(value, bit)
        return value, more

    own, own_more = poled(swept_own, x_own)
    theirs, theirs_more = poled(swept_theirs, x_theirs)
    total, packed, packed_send = scratch(
        gram_kernel, [(2, vectors, columns // 2), (half, vectors), (half, vectors)],
        [(vectors, vectors)], own, own_more, theirs, theirs_more,
    )
    packed = packed + over_poles(packed_send, 0)
    for bit in range(devices.bit_length() - 1):
        mask = (2 << bit) - 2 if bit else 1
        packed = packed + lax.ppermute(
            packed, "rows", [(place, place ^ mask) for place in range(devices)]
        )
    packed_theirs = over_poles(packed, 0)
    total_theirs = over_poles(total, 0)
    q_high, q_low = pl.pallas_call(
        parts_kernel,
        out_shape=[jax.ShapeDtypeStruct((2,) + total.shape, jnp.bfloat16)] * 2,
        in_specs=[pl.BlockSpec(memory_space=vmem)] * 2,
        out_specs=[pl.BlockSpec(memory_space=vmem)] * 2,
        compiler_params=pltpu.CompilerParams(vmem_limit_bytes=GRANT),
    )(total, total_theirs)
    (result,) = scratch(
        functools.partial(finish_kernel, float(columns * devices)),
        [(2, vectors // poles, columns)], [(vectors, vectors), state],
        packed, packed_theirs, q_high, q_low, products=4,
    )
    return result


def solution(mesh):
    placed = (
        P(None, None, "rows"),
        P("pole", "rows", None, None, None),
        P("pole", "rows", None, None, None),
        P("pole", "rows", None, None, None),
        P("pole", None),
    )
    return jax.shard_map(
        shards, mesh=mesh, in_specs=placed, out_specs=P(None, "pole", "rows"), check_vma=False
    )
```

```python
import functools

import jax
import jax.numpy as jnp
from jax import lax
from jax.experimental import pallas as pl
from jax.experimental.pallas import tpu as pltpu
from jax.sharding import PartitionSpec as P


GRANT = 8 << 20
LANES = 128
HIGH = lax.Precision.HIGH
F32 = jnp.float32


def dot(a, b, dims, precision=None):
    return lax.dot_general(
        a, b, (dims, ((), ())), precision=precision, preferred_element_type=F32
    )


def halves(a):
    high = a.astype(jnp.bfloat16)
    return high, (a - high.astype(F32)).astype(jnp.bfloat16)


def stacked(value):
    real, imag = halves(value[0]), halves(value[1])
    high = jnp.concatenate([real[0], imag[0]], axis=0)
    return high, jnp.concatenate([high, real[1], imag[1]], axis=0)


def against(left, part, dims):
    high, both = left
    size = high.shape[0]
    wide = dot(both, part[0], dims)
    value = wide[:size] + (wide[size:] + dot(high, part[1], dims))
    return value[: size // 2], value[size // 2 :]


def few(left, parts, dims):
    return few_stacked(stacked(left), parts, dims)


def few_stacked(left, parts, dims):
    with_real, with_imag = against(left, parts[0], dims), against(left, parts[1], dims)
    return with_real[0] - with_imag[1], with_imag[0] + with_real[1]


def times(left, right, dims):
    rows = left[0].shape[0]
    if rows <= LANES // 2 or (rows <= LANES and dims[1] == (1,)):
        return few(left, (halves(right[0]), halves(right[1])), dims)
    real = dot(left[0], right[0], dims, HIGH) - dot(left[1], right[1], dims, HIGH)
    imag = dot(left[0], right[1], dims, HIGH) + dot(left[1], right[0], dims, HIGH)
    return real, imag


def plain(left, right):
    return times(left, right, ((1,), (0,)))


def trans(left, right):
    return times(left, right, ((1,), (1,)))


def plus(a, b):
    return a[0] + b[0], a[1] + b[1]


def minus(a, b):
    return a[0] - b[0], a[1] - b[1]


def negative(a):
    return -a[0], -a[1]


def pick(choice, a, b):
    return jnp.where(choice, a[0], b[0]), jnp.where(choice, a[1], b[1])


def pair(ref, *index):
    return ref[(*index, 0)], ref[(*index, 1)]


def put(ref, value):
    ref[0] = value[0]
    ref[1] = value[1]


def rows_of(ref, start, size):
    start = pl.multiple_of(start, size)
    return ref[0, pl.ds(start, size), :], ref[1, pl.ds(start, size), :]


def call(body, outs, *args, products=1):
    shapes = [jax.ShapeDtypeStruct(shape, F32) for shape in outs]
    return pl.pallas_call(
        body,
        out_shape=shapes,
        in_specs=[pl.BlockSpec(memory_space=pltpu.VMEM)] * len(args),
        out_specs=[pl.BlockSpec(memory_space=pltpu.VMEM)] * len(outs),
        cost_estimate=pl.CostEstimate(
            flops=products * 3 * 8 * 256**3, bytes_accessed=1 << 20, transcendentals=0
        ),
        compiler_params=pltpu.CompilerParams(vmem_limit_bytes=GRANT),
    )(*args)


def side():
    return lax.rem(lax.axis_index("rows"), 2) == 0


def map_kernel(lower, out):
    count = lower.shape[0]
    value = pair(lower, 0)
    for number in range(1, count):
        value = plain(pair(lower, number), value)
    if count % 2:
        value = negative(value)
    put(out, value)


def local_kernel(piece, pivot, lower, upper, ahead, states, bkeep, bsend, gkeep, cmap, cmaps, late, work):
    count, width = pivot.shape[0], pivot.shape[-1]
    half = bkeep.shape[1]
    mine = jnp.where(side(), 0, half)
    other = half - mine
    last = None
    for number in range(count):
        columns = slice(number * width, (number + 1) * width)
        value = trans((piece[0, :, columns], piece[1, :, columns]), pair(pivot, number))
        if last is not None:
            value = minus(value, trans(last, pair(lower, number)))
        states[number, 0] = value[0]
        states[number, 1] = value[1]
        last = value
    put(bkeep, rows_of(states.at[count - 1], mine, half))
    put(bsend, rows_of(states.at[count - 1], other, half))
    for number in range(count - 2, -1, -1):
        last = minus(pair(states, number), trans(last, pair(upper, number)))
    put(work, last)
    put(gkeep, rows_of(work, mine, half))
    value = rows_of(work, other, half)
    for part in range(2):
        late[part, width:, :] = value[part]
    levels = [negative(pair(lower, 0))]
    for number in range(1, count - 1):
        levels.append(negative(plain(pair(lower, number), levels[-1])))
    if count > 1:
        levels.append(pair(ahead))
    value = levels[-1]
    for number in range(count - 2, -1, -1):
        value = minus(levels[number], plain(pair(upper, number), value))
    for part in range(2):
        late[part, :width, :] = value[part]
    value = negative(pair(upper, count - 1))
    put(cmaps.at[count - 1], value)
    for number in range(count - 2, -1, -1):
        value = negative(plain(pair(upper, number), value))
        put(cmaps.at[number], value)
    put(cmap, value)


def part_of(ref, start, size):
    return ref[0, start : start + size, :], ref[1, start : start + size, :]


def join_kernel(mine, theirs, bmine, btheirs, out_b, out_a):
    first = side()
    a_first = pick(first, pair(mine), pair(theirs))
    a_second = pick(first, pair(theirs), pair(mine))
    b_first = pick(first, pair(bmine), pair(btheirs))
    b_second = pick(first, pair(btheirs), pair(bmine))
    put(out_b, plus(trans(b_first, a_second), b_second))
    put(out_a, plain(a_second, a_first))


def join_back_kernel(mine, theirs, out):
    first = side()
    c_first = pick(first, pair(mine), pair(theirs))
    c_second = pick(first, pair(theirs), pair(mine))
    put(out, plain(c_first, c_second))


def apply_kernel(state, matrix, base, out):
    put(out, plus(trans(pair(state), pair(matrix)), pair(base)))


def enter_kernel(inflow, a_mine, a_theirs, b_mine, b_theirs, in_own, in_other):
    first = side()
    entering = pair(inflow)
    a_first = pick(first, pair(a_mine), pair(a_theirs))
    second = plus(trans(entering, a_first), pick(first, pair(b_mine), pair(b_theirs)))
    put(in_own, pick(first, entering, second))
    put(in_other, pick(first, second, entering))


def turn_kernel(in_own, in_other, g_mine, late_mine, late_theirs, c_mine, c_theirs, mid, *outs):
    first = side()
    size = c_mine.shape[1]
    half = in_own.shape[1]
    entering = pick(first, pair(in_own), pair(in_other))
    second = pick(first, pair(in_other), pair(in_own))
    r_mine, r_theirs = part_of(late_mine, 0, size), part_of(late_theirs, 0, size)
    g_own, g_theirs = pair(g_mine), part_of(late_theirs, size, half)
    middle = plus(pick(first, g_theirs, g_own), trans(second, pick(first, r_theirs, r_mine)))
    put(mid, middle)
    value = plus(pick(first, g_own, g_theirs), trans(entering, pick(first, r_mine, r_theirs)))
    value = plus(value, trans(middle, pick(first, pair(c_mine), pair(c_theirs))))
    if len(outs) == 1:
        put(outs[0], value)
        return
    quarter = half // 2
    low = (value[0][:quarter], value[1][:quarter])
    high = (value[0][quarter:], value[1][quarter:])
    source = back_place(4) == 0
    put(outs[0], pick(source, low, high))
    put(outs[1], pick(source, high, low))


def back_place(nodes):
    return nodes - 1 - lax.div(lax.axis_index("rows"), 2)


def middle_kernel(mine_a, mine_b, came_a, came_b, c_mine, c_other, keep, send, last):
    place = back_place(4)
    one = place == 1
    c_one = pick(one, pair(c_mine), pair(c_other))
    c_two = pick(one, pair(c_other), pair(c_mine))
    start = pick(one, pair(came_a), pair(came_b))
    second = plus(trans(start, c_one), pick(one, pair(mine_b), pair(came_a)))
    third = plus(trans(second, c_two), pick(one, pair(came_b), pair(mine_a)))
    put(keep, pick(one, start, second))
    put(send, pick(place == 0, pair(mine_b), pick(one, second, third)))
    put(last, third)


def back_in(entering, mid, c_mine, c_theirs, own, other):
    first = side()
    first_in = plus(pair(mid), trans(entering, pick(first, pair(c_theirs), pair(c_mine))))
    put(own, pick(first, first_in, entering))
    put(other, pick(first, entering, first_in))


def back_in_kernel(back_inflow, *refs):
    back_in(pair(back_inflow), *refs)


def back_in_parts_kernel(keep, came, last, mid, c_mine, c_theirs, own, other, work):
    place = back_place(4)
    low = pick(place == 1, pair(keep), pick(place == 2, pair(came), pair(last)))
    high = pick(place == 2, pair(keep), pair(came))
    quarter = keep.shape[1]
    for part in range(2):
        work[part, :quarter] = low[part]
        work[part, quarter:] = high[part]
    back_in(pair(work), mid, c_mine, c_theirs, own, other)


def swept_kernel(states, in_own, in_theirs, lower, upper, c_maps, weights, out_own, out_theirs):
    count = states.shape[0]
    half = in_own.shape[1]
    mine = jnp.where(side(), 0, half)
    for carry, start, out in ((in_own, mine, out_own), (in_theirs, half - mine, out_theirs)):
        carry = pair(carry)
        for number in range(count):
            carry = negative(trans(carry, pair(lower, number)))
            value = plus(rows_of(states.at[number], start, half), carry)
            put(out.at[number], value)
        for number in range(count - 2, -1, -1):
            value = minus(pair(out, number), trans(value, pair(upper, number)))
            put(out.at[number], value)


def solved_kernel(swept, entering, c_maps, weights, keep, send):
    count, width = swept.shape[0], swept.shape[-1]
    wreal, wimag = weights[0, 0], weights[0, 1]
    left = stacked(pair(entering))
    upward = lax.rem(lax.axis_index("pole"), 2) == 1
    values = []
    for number in range(count):
        maps = pair(c_maps, number)
        product = few_stacked(left, (halves(maps[0]), halves(maps[1])), ((1,), (1,)))
        value = plus(pair(swept, number), product)
        values.append((wreal * value[0] - wimag * value[1], wreal * value[1] + wimag * value[0]))
    blocks = count // 2
    for number in range(blocks):
        columns = slice(number * width, (number + 1) * width)
        for part in range(2):
            low, high = values[number][part], values[number + blocks][part]
            keep[part, :, columns] = jnp.where(upward, high, low)
            send[part, :, columns] = jnp.where(upward, low, high)


def gram_kernel(own, own_more, theirs, theirs_more, total, keep, send, work):
    size = total.shape[1]
    half = size // 2
    mine = jnp.where(side(), 0, half)
    for first, second, start in ((own, own_more, mine), (theirs, theirs_more, half - mine)):
        start = pl.multiple_of(start, half)
        for part in range(2):
            total[part, pl.ds(start, half), :] = first[part] + second[part]
    basis = pair(total)
    dims = ((1,), (1,))
    real = dot(basis[0], basis[0], dims, HIGH) + dot(basis[1], basis[1], dims, HIGH)
    imag = dot(basis[0], basis[1], dims, HIGH) - dot(basis[1], basis[0], dims, HIGH)
    row = lax.broadcasted_iota(jnp.int32, (size, size), 0)
    column = lax.broadcasted_iota(jnp.int32, (size, size), 1)
    work[...] = jnp.where(row <= column, real, imag)
    start = pl.multiple_of(lax.rem(lax.axis_index("pole"), 2) * half, half)
    keep[...] = work[pl.ds(start, half), :]
    send[...] = work[pl.ds(pl.multiple_of(half - start, half), half), :]


def parts_kernel(mine, theirs, high, low):
    for number, piece in enumerate((mine, theirs)):
        for part in range(2):
            high[number, part], low[number, part] = halves(piece[part])


def finish_kernel(states, mine, theirs, q_high, q_low, out, held, slab):
    size = held.shape[0]
    half = size // 2
    columns = out.shape[1]
    pole = lax.axis_index("pole")
    start = pl.multiple_of(lax.rem(pole, 2) * half, half)
    held[pl.ds(start, half), :] = mine[...]
    held[pl.ds(pl.multiple_of(half - start, half), half), :] = theirs[...]
    packed = held[...]
    turned = packed.T
    row = lax.broadcasted_iota(jnp.int32, (size, size), 0)
    column = lax.broadcasted_iota(jnp.int32, (size, size), 1)
    real = jnp.where(row <= column, packed, turned)
    imag = jnp.where(row < column, turned, jnp.where(row > column, -packed, 0.0))
    frob = jnp.sqrt(jnp.sum(real * real + imag * imag, keepdims=True))
    scale = 1.0 / frob
    current = (real * scale, imag * scale)
    put(slab, current)
    factor = (jnp.where(row == column, 1.5, 0.0) - 0.5 * current[0], -0.5 * current[1])
    factor = (halves(factor[0]), halves(factor[1]))
    dims = ((1,), (0,))
    place = pl.multiple_of(pole * columns, columns)
    strip = (slab[0, pl.ds(place, columns), :], slab[1, pl.ds(place, columns), :])
    strip = few(few(strip, factor, dims), factor, dims)
    on = lax.broadcasted_iota(jnp.int32, strip[0].shape, 0) + place
    on = on == lax.broadcasted_iota(jnp.int32, strip[0].shape, 1)
    strip = (jnp.where(on, 1.5, 0.0) - 0.5 * strip[0], -0.5 * strip[1])
    mixing = few(strip, factor, dims)
    factor = jnp.sqrt(states / frob)
    mixing = (mixing[0] * factor, mixing[1] * factor)
    width = q_high.shape[3]
    place = lax.rem(pole, 2) * width
    for number, offset in enumerate((place, width - place)):
        parts = tuple((q_high[number, part], q_low[number, part]) for part in range(2))
        value = few(mixing, parts, dims)
        for part in range(2):
            out[part, :, pl.ds(pl.multiple_of(offset, width), width)] = value[part]


def shards(subspace, pivots, lower_blocks, upper_blocks, pole_weights):
    devices = lax.axis_size("rows")
    poles = lax.axis_size("pole")
    count, width = pivots.shape[1], pivots.shape[-1]
    vectors = subspace.shape[1]
    half = vectors // 2
    nodes = devices // 2
    pivot, lower, upper = pivots[0], lower_blocks[0], upper_blocks[0]
    square = (2, width, width)
    state = (2, vectors, width)
    strip = (2, half, width)
    vmem = pltpu.VMEM

    def scratch(body, outs, extra, *args, products=1):
        return pl.pallas_call(
            body,
            out_shape=[jax.ShapeDtypeStruct(shape, F32) for shape in outs],
            in_specs=[pl.BlockSpec(memory_space=vmem)] * len(args),
            out_specs=[pl.BlockSpec(memory_space=vmem)] * len(outs),
            scratch_shapes=[vmem(shape, F32) for shape in extra],
            cost_estimate=pl.CostEstimate(
                flops=products * 3 * 8 * 256**3, bytes_accessed=1 << 20, transcendentals=0
            ),
            compiler_params=pltpu.CompilerParams(vmem_limit_bytes=GRANT),
        )(*args)

    swap = [(place, place ^ 1) for place in range(devices)]

    def beside(value):
        return lax.ppermute(value, "rows", swap)

    def between(value, moves):
        return lax.ppermute(
            value, "rows", [(2 * a + s, 2 * b + s) for a, b in moves for s in range(2)]
        )

    def prefix(base, matrix, order):
        inflow = None
        for hop in range(nodes - 1):
            passed = base
            if hop:
                (passed,) = call(apply_kernel, [strip], inflow, matrix, base)
            came = between(passed, [(order[hop], order[hop + 1])])
            inflow = came if inflow is None else inflow + came
        return jnp.zeros(strip, F32) if inflow is None else inflow

    (a_mine,) = call(map_kernel, [square], lower)
    a_theirs = beside(a_mine)
    states, b_mine, b_send, g_mine, c_mine, c_maps, late_mine = scratch(
        local_kernel,
        [(count,) + state, strip, strip, strip, square, (count,) + square,
         (2, width + half, width)],
        [state], subspace, pivot, lower, upper, a_mine, products=2 * count + 3,
    )
    b_theirs = beside(b_send)
    c_theirs = beside(c_mine)
    late_theirs = beside(late_mine)

    b_node, a_node = call(join_kernel, [strip, square], a_mine, a_theirs, b_mine, b_theirs)
    order = list(range(nodes))
    inflow = prefix(b_node, a_node, order)
    (c_node,) = call(join_back_kernel, [square], c_mine, c_theirs)
    quarter = (2, half // 2, width)
    short = nodes == 4
    in_own, in_other = call(enter_kernel, [strip] * 2, inflow, a_mine, a_theirs, b_mine, b_theirs)
    in_theirs = beside(in_other)
    mid, *ends = call(
        turn_kernel, [strip] + ([quarter] * 2 if short else [strip]), in_own, in_other,
        g_mine, late_mine, late_theirs, c_mine, c_theirs, products=2,
    )
    if short:
        c_other = between(c_node, [(1, 2), (2, 1)])
        came_a = between(ends[0], [(3, 2), (2, 1)])
        came_b = between(ends[1], [(3, 1), (1, 2)])
        keep, send, last = call(
            middle_kernel, [quarter] * 3, *ends, came_a, came_b, c_node, c_other
        )
        came = between(send, [(3, 2), (2, 1), (1, 0)])
        last = between(last, [(2, 0)])
    else:
        back_inflow = prefix(ends[0], c_node, order[::-1])
    swept_own, swept_theirs = pl.pallas_call(
        swept_kernel,
        out_shape=[jax.ShapeDtypeStruct((count,) + strip, F32)] * 2,
        in_specs=[pl.BlockSpec(memory_space=vmem)] * 6
        + [pl.BlockSpec(memory_space=pltpu.SMEM)],
        out_specs=[pl.BlockSpec(memory_space=vmem)] * 2,
        compiler_params=pltpu.CompilerParams(vmem_limit_bytes=GRANT),
    )(states, in_own, in_theirs, lower, upper, c_maps, pole_weights)
    if short:
        x_own, x_other = scratch(
            back_in_parts_kernel, [strip] * 2, [strip], keep, came, last, mid, c_mine, c_theirs
        )
    else:
        x_own, x_other = call(
            back_in_kernel, [strip] * 2, back_inflow, mid, c_mine, c_theirs
        )
    x_theirs = beside(x_other)

    def over_poles(value, bit):
        return lax.ppermute(value, "pole", [(place, place ^ (1 << bit)) for place in range(poles)])

    levels = poles.bit_length() - 1
    columns = count * width
    block = (2, half, columns // 2)

    def poled(swept, entering):
        keep, send = pl.pallas_call(
            solved_kernel,
            out_shape=[jax.ShapeDtypeStruct(block, F32)] * 2,
            in_specs=[pl.BlockSpec(memory_space=vmem)] * 3
            + [pl.BlockSpec(memory_space=pltpu.SMEM)],
            out_specs=[pl.BlockSpec(memory_space=vmem)] * 2,
            compiler_params=pltpu.CompilerParams(vmem_limit_bytes=GRANT),
        )(swept, entering, c_maps, pole_weights)
        value, more = keep, over_poles(send, 0)
        for bit in range(1, levels):
            value = value + more
            more = over_poles(value, bit)
        return value, more

    own, own_more = poled(swept_own, x_own)
    theirs, theirs_more = poled(swept_theirs, x_theirs)
    total, packed, packed_send = scratch(
        gram_kernel, [(2, vectors, columns // 2), (half, vectors), (half, vectors)],
        [(vectors, vectors)], own, own_more, theirs, theirs_more,
    )
    packed = packed + over_poles(packed_send, 0)
    for bit in range(devices.bit_length() - 1):
        mask = 1 << bit
        packed = packed + lax.ppermute(
            packed, "rows", [(place, place ^ mask) for place in range(devices)]
        )
    packed_theirs = over_poles(packed, 0)
    total_theirs = over_poles(total, 0)
    q_high, q_low = pl.pallas_call(
        parts_kernel,
        out_shape=[jax.ShapeDtypeStruct((2,) + total.shape, jnp.bfloat16)] * 2,
        in_specs=[pl.BlockSpec(memory_space=vmem)] * 2,
        out_specs=[pl.BlockSpec(memory_space=vmem)] * 2,
        compiler_params=pltpu.CompilerParams(vmem_limit_bytes=GRANT),
    )(total, total_theirs)
    (result,) = scratch(
        functools.partial(finish_kernel, float(columns * devices)),
        [(2, vectors // poles, columns)], [(vectors, vectors), state],
        packed, packed_theirs, q_high, q_low, products=4,
    )
    return result


def solution(mesh):
    placed = (
        P(None, None, "rows"),
        P("pole", "rows", None, None, None),
        P("pole", "rows", None, None, None),
        P("pole", "rows", None, None, None),
        P("pole", None),
    )
    return jax.shard_map(
        shards, mesh=mesh, in_specs=placed, out_specs=P(None, "pole", "rows"), check_vma=False
    )
```
